32 devices in a mesh: dp: 1 (over z), fsdp: 32 (over y, x, core).
Axes of the slice: x: 4, y: 4, z: 1, core: 2. Of those that a mesh axis runs over, the one named last changes fastest.
The devices are a block of a 4x4x8 slice.
Arguments:
- hidden: bfloat16 [32, 256, 2048], P(('dp', 'fsdp'))
- doc_lens: int32 [32], P(('dp', 'fsdp'))
- ln_par: float32 [2, 4, 2048], P(None, None, 'fsdp')
- w_qkv: bfloat16 [2, 2048, 16, 384], P(None, 'fsdp')
- b_qkv: bfloat16 [2, 6144], P(None, 'fsdp')
- w_out: bfloat16 [2, 2048, 2048], P(None, 'fsdp')
- b_out: bfloat16 [2, 2048], P(None, 'fsdp')
- w_up: bfloat16 [2, 2048, 8192], P(None, 'fsdp')
- b_up: bfloat16 [2, 8192], P(None, 'fsdp')
- w_down: bfloat16 [2, 8192, 2048], P(None, 'fsdp')
- b_down: bfloat16 [2, 2048], P(None, 'fsdp')
Outputs:
- output: bfloat16 [32, 256, 2048], P(('dp', 'fsdp'))
All inputs are finite; a program needn't handle non-finite values.
Results may differ from the reference program's by a relative error of at most 0.00791475.
Values are sent between devices in bfloat16 or wider.
A program may use at most 768 MiB of HBM per device.

```python
import jax
import jax.numpy as jnp
from jax import lax

D_MODEL = 2048
NUM_HEADS = 16
HEAD_DIM = 128
FF_DIM = 8192
SEQ_LEN = 256
NUM_DOCS = 32
NUM_LAYERS = 2
ROT_DIM = HEAD_DIM // 4
ROPE_BASE = 10000.0
LN_EPS = 1e-5


def setup_inputs(seed: int = 0, part: int = 0) -> dict:
    shared_key, doc_root = jax.random.split(jax.random.key(seed))
    part_key = jax.random.fold_in(doc_root, part)
    hidden_key, lens_key = jax.random.split(part_key)
    w_keys = jax.random.split(shared_key, 9)
    hidden = jax.random.normal(hidden_key, (NUM_DOCS, SEQ_LEN, D_MODEL), jnp.float32).astype(jnp.bfloat16)
    drawn_lens = jax.random.randint(lens_key, (NUM_DOCS,), 1, SEQ_LEN + 1, jnp.int32)
    doc_lens = drawn_lens.at[0].set(SEQ_LEN)
    ln_offset = jnp.array([1.0, 0.0, 1.0, 0.0], jnp.float32)[None, :, None]
    ln_par = ln_offset + 0.4 * jax.random.normal(w_keys[0], (NUM_LAYERS, 4, D_MODEL), jnp.float32)
    w_qkv = (jax.random.normal(w_keys[1], (NUM_LAYERS, D_MODEL, NUM_HEADS, 3 * HEAD_DIM), jnp.float32) * D_MODEL ** -0.5).astype(jnp.bfloat16)
    b_qkv = (0.5 * jax.random.normal(w_keys[2], (NUM_LAYERS, 3 * D_MODEL), jnp.float32)).astype(jnp.bfloat16)
    w_out = (jax.random.normal(w_keys[3], (NUM_LAYERS, D_MODEL, D_MODEL), jnp.float32) * D_MODEL ** -0.5).astype(jnp.bfloat16)
    b_out = (0.5 * jax.random.normal(w_keys[4], (NUM_LAYERS, D_MODEL), jnp.float32)).astype(jnp.bfloat16)
    w_up = (jax.random.normal(w_keys[5], (NUM_LAYERS, D_MODEL, FF_DIM), jnp.float32) * D_MODEL ** -0.5).astype(jnp.bfloat16)
    b_up = (0.5 * jax.random.normal(w_keys[6], (NUM_LAYERS, FF_DIM), jnp.float32)).astype(jnp.bfloat16)
    w_down = (jax.random.normal(w_keys[7], (NUM_LAYERS, FF_DIM, D_MODEL), jnp.float32) * FF_DIM ** -0.5).astype(jnp.bfloat16)
    b_down = (0.5 * jax.random.normal(w_keys[8], (NUM_LAYERS, D_MODEL), jnp.float32)).astype(jnp.bfloat16)
    return {'hidden': hidden, 'doc_lens': doc_lens, 'ln_par': ln_par, 'w_qkv': w_qkv, 'b_qkv': b_qkv, 'w_out': w_out, 'b_out': b_out, 'w_up': w_up, 'b_up': b_up, 'w_down': w_down, 'b_down': b_down}


def layer_norm(row_vals, gain_vec, shift_vec):
    mean_vals = jnp.mean(row_vals, axis=-1, keepdims=True)
    centered = row_vals - mean_vals
    var_vals = jnp.mean(centered * centered, axis=-1, keepdims=True)
    normed = centered * lax.rsqrt(var_vals + LN_EPS)
    return (normed * gain_vec + shift_vec).astype(jnp.bfloat16)


def rotary_tables(seq_len, rot_dim):
    inv_freq = 1.0 / (ROPE_BASE ** (jnp.arange(0, rot_dim, 2, dtype=jnp.float32) / rot_dim))
    angles = jnp.arange(seq_len, dtype=jnp.float32)[:, None] * inv_freq[None, :]
    angles = jnp.concatenate([angles, angles], axis=-1)
    return jnp.cos(angles), jnp.sin(angles)


def apply_rotary(head_vals, cos_tab, sin_tab):
    half_rot = ROT_DIM // 2
    rot_part = head_vals[..., :ROT_DIM].astype(jnp.float32)
    turned = jnp.concatenate([-rot_part[..., half_rot:], rot_part[..., :half_rot]], axis=-1)
    rotated = rot_part * cos_tab[:, None, :] + turned * sin_tab[:, None, :]
    return jnp.concatenate([rotated.astype(jnp.bfloat16), head_vals[..., ROT_DIM:]], axis=-1)


def doc_forward(doc_hidden, doc_len, layer_params, cos_tab, sin_tab):
    positions = jnp.arange(SEQ_LEN)
    visible = (positions[None, :] <= positions[:, None]) & (positions[None, :] < doc_len)

    def layer_step(x_cur, params):
        ln_rows, w_qkv_l, b_qkv_l, w_out_l, b_out_l, w_up_l, b_up_l, w_down_l, b_down_l = params
        x_rows = x_cur.astype(jnp.float32)
        attn_in = layer_norm(x_rows, ln_rows[0], ln_rows[1])
        mlp_in = layer_norm(x_rows, ln_rows[2], ln_rows[3])
        qkv_rows = jnp.dot(attn_in, w_qkv_l.reshape(D_MODEL, 3 * D_MODEL), preferred_element_type=jnp.float32) + b_qkv_l.astype(jnp.float32)
        qkv_heads = qkv_rows.astype(jnp.bfloat16).reshape(SEQ_LEN, NUM_HEADS, 3 * HEAD_DIM)
        queries = apply_rotary(qkv_heads[:, :, :HEAD_DIM], cos_tab, sin_tab)
        keys_rot = apply_rotary(qkv_heads[:, :, HEAD_DIM:2 * HEAD_DIM], cos_tab, sin_tab)
        values = qkv_heads[:, :, 2 * HEAD_DIM:]
        scores = jnp.einsum('qhe,khe->hqk', queries.astype(jnp.float32), keys_rot.astype(jnp.float32)) * (HEAD_DIM ** -0.5)
        prob_bf = jax.nn.softmax(jnp.where(visible[None], scores, -1e30), axis=-1).astype(jnp.bfloat16)
        context = jnp.einsum('hqk,khe->qhe', prob_bf.astype(jnp.float32), values.astype(jnp.float32))
        context = context.astype(jnp.bfloat16).reshape(SEQ_LEN, D_MODEL)
        attn_out = jnp.dot(context, w_out_l, preferred_element_type=jnp.float32) + b_out_l.astype(jnp.float32)
        up_rows = jnp.dot(mlp_in, w_up_l, preferred_element_type=jnp.float32) + b_up_l.astype(jnp.float32)
        act_rows = jax.nn.gelu(up_rows, approximate=False).astype(jnp.bfloat16)
        mlp_out = jnp.dot(act_rows, w_down_l, preferred_element_type=jnp.float32) + b_down_l.astype(jnp.float32)
        new_x = (x_rows + attn_out + mlp_out).astype(jnp.bfloat16)
        return new_x, None

    return lax.scan(layer_step, doc_hidden, layer_params)[0]


def reference(hidden, doc_lens, ln_par, w_qkv, b_qkv, w_out, b_out, w_up, b_up, w_down, b_down):
    cos_tab, sin_tab = rotary_tables(SEQ_LEN, ROT_DIM)
    layer_params = (ln_par, w_qkv, b_qkv, w_out, b_out, w_up, b_up, w_down, b_down)
    return lax.map(lambda doc_item: doc_forward(doc_item[0], doc_item[1], layer_params, cos_tab, sin_tab), (hidden, doc_lens))
```

```python
import functools
import math

import jax
import jax.numpy as jnp
from jax import lax
from jax.experimental import pallas as pl
from jax.experimental.pallas import tpu as pltpu
from jax.sharding import PartitionSpec as P

ROPE_BASE = 10000.0
LN_EPS = 1e-5
CORES = 2
MESH = pl.DeviceIdType.MESH


def layer_norm(row_vals, gain_vec, shift_vec):
    mean_vals = jnp.mean(row_vals, axis=-1, keepdims=True)
    centered = row_vals - mean_vals
    var_vals = jnp.mean(centered * centered, axis=-1, keepdims=True)
    normed = centered * lax.rsqrt(var_vals + LN_EPS)
    return (normed * gain_vec + shift_vec).astype(jnp.bfloat16)


def rotary_tables(seq_len, rot_dim):
    inv_freq = 1.0 / (ROPE_BASE ** (jnp.arange(0, rot_dim, 2, dtype=jnp.float32) / rot_dim))
    angles = jnp.arange(seq_len, dtype=jnp.float32)[:, None] * inv_freq[None, :]
    angles = jnp.concatenate([angles, angles], axis=-1)
    return jnp.cos(angles), jnp.sin(angles)


def apply_rotary(head_vals, cos_tab, sin_tab):
    rot_dim = cos_tab.shape[-1]
    half_rot = rot_dim // 2
    rot_part = head_vals[..., :rot_dim].astype(jnp.float32)
    turned = jnp.concatenate([-rot_part[..., half_rot:], rot_part[..., :half_rot]], axis=-1)
    rotated = rot_part * cos_tab[:, None, :] + turned * sin_tab[:, None, :]
    return jnp.concatenate([rotated.astype(jnp.bfloat16), head_vals[..., rot_dim:]], axis=-1)


def attention_core(qkv_heads, lens_loc):
    num_docs, seq_len, num_heads, triple = qkv_heads.shape
    head_dim = triple // 3
    cos_tab, sin_tab = rotary_tables(seq_len, head_dim // 4)
    queries = apply_rotary(qkv_heads[..., :head_dim], cos_tab, sin_tab)
    keys_rot = apply_rotary(qkv_heads[..., head_dim:2 * head_dim], cos_tab, sin_tab)
    values = qkv_heads[..., 2 * head_dim:]
    scores = jnp.einsum('nqhe,nkhe->nhqk', queries, keys_rot, preferred_element_type=jnp.float32) * (head_dim ** -0.5)
    positions = jnp.arange(seq_len)
    causal = positions[None, :] <= positions[:, None]
    visible = causal[None, None] & (positions[None, None, None, :] < lens_loc[:, None, None, None])
    prob_bf = jax.nn.softmax(jnp.where(visible, scores, -1e30), axis=-1).astype(jnp.bfloat16)
    context = jnp.einsum('nhqk,nkhe->nqhe', prob_bf, values, preferred_element_type=jnp.float32)
    return context.astype(jnp.bfloat16).reshape(num_docs * seq_len, num_heads * head_dim)


def layer_partial(docs, lens_grp, ln_full, w_qkv, b_qkv, w_out, w_up, b_up, w_down, head_dim):
    num_docs, seq_len, d_model = docs.shape
    x_rows = docs.reshape(num_docs * seq_len, d_model).astype(jnp.float32)
    attn_in = layer_norm(x_rows, ln_full[0], ln_full[1])
    mlp_in = layer_norm(x_rows, ln_full[2], ln_full[3])
    qkv_rows = jnp.dot(attn_in, w_qkv, preferred_element_type=jnp.float32) + b_qkv
    qkv_heads = qkv_rows.astype(jnp.bfloat16).reshape(num_docs, seq_len, -1, 3 * head_dim)
    context = attention_core(qkv_heads, lens_grp)
    up_rows = jnp.dot(mlp_in, w_up, preferred_element_type=jnp.float32) + b_up
    act_rows = jax.nn.gelu(up_rows, approximate=False).astype(jnp.bfloat16)
    total = jnp.dot(context, w_out, preferred_element_type=jnp.float32) + jnp.dot(act_rows, w_down, preferred_element_type=jnp.float32)
    return total.reshape(num_docs, seq_len, d_model)


def send(src, dst, send_sem, recv_sem, dev):
    copy = pltpu.make_async_remote_copy(src_ref=src, dst_ref=dst, send_sem=send_sem, recv_sem=recv_sem, device_id={"fsdp": dev}, device_id_type=MESH)
    copy.start()
    return copy


def arrived(dst, sem):
    pltpu.make_async_copy(dst, dst, sem).wait()


class Place:
    def __init__(self, side):
        me = lax.axis_index("fsdp")
        self.side, self.me = side, me
        self.core = lax.rem(me, CORES)
        self.col = lax.rem(me // CORES, side)
        self.row = me // (CORES * side)
        self.sib = self.dev(self.row, self.col, 1 - self.core)

    def dev(self, row, col, core):
        return (row * self.side + col) * CORES + core

    def step(self, pos, by):
        return lax.rem(pos + by + self.side, self.side)

    def in_row(self, by):
        return self.dev(self.row, self.step(self.col, by), self.core)

    def in_col(self, by):
        return self.dev(self.step(self.row, by), self.col, self.core)


class Ring:
    def __init__(self, pos, place, right, left, blk, own, ss, rs):
        self.pos, self.right, self.left, self.blk, self.own, self.ss, self.rs = pos, right, left, blk, own, ss, rs
        self.prev, self.next, self.far = place.step(pos, -1), place.step(pos, 1), place.step(pos, 2)
        self.sent = []

    def _send(self, src, pos, half, i, j, dev):
        self.sent.append(send(src, self.blk(pos, half), self.ss.at[i], self.rs.at[j], dev))

    def start(self):
        self._send(self.own(0), self.pos, 0, 0, 0, self.right)
        self._send(self.own(1), self.pos, 1, 2, 3, self.left)
        self._send(self.own(1), self.pos, 1, 1, 1, self.right)
        self._send(self.own(0), self.pos, 0, 3, 2, self.left)

    def forward(self):
        arrived(self.blk(self.prev, 0), self.rs.at[0])
        self._send(self.blk(self.prev, 0), self.prev, 0, 4, 4, self.right)
        arrived(self.blk(self.next, 1), self.rs.at[3])
        self._send(self.blk(self.next, 1), self.next, 1, 5, 5, self.left)

    def rest(self):
        arrived(self.blk(self.prev, 1), self.rs.at[1])
        arrived(self.blk(self.next, 0), self.rs.at[2])

    def last(self):
        arrived(self.blk(self.far, 0), self.rs.at[4])
        arrived(self.blk(self.far, 1), self.rs.at[5])

    def drain(self):
        for copy in self.sent:
            copy.wait_send()


class Pair:
    def __init__(self, ring, place, theirs, cs, cr):
        self.ring, self.place, self.theirs, self.cs, self.cr, self.sent = ring, place, theirs, cs, cr, []
        self.blocks = (ring.pos, ring.prev, ring.next, ring.far)

    def give(self, rel, half, src=None):
        i = rel * 2 + half
        blk = self.ring.blk(self.blocks[rel], half)
        self.sent.append(send(blk if src is None else src, blk, self.cs.at[i], self.cr.at[i], self.place.sib))

    def take(self):
        for rel in range(4):
            for half in range(2):
                arrived(self.theirs(self.blocks[rel], half), self.cr.at[rel * 2 + half])

    def drain(self):
        for copy in self.sent:
            copy.wait_send()


def meet(place, devices):
    barrier = pltpu.get_barrier_semaphore()
    for dev in devices:
        pl.semaphore_signal(barrier, inc=1, device_id={"fsdp": dev}, device_id_type=MESH)
    pl.semaphore_wait(barrier, len(devices))


def weight_gather(place, specs, sems):
    ss, rs, cs, cr = sems
    out = []
    for t, (blk, own) in enumerate(specs):
        mine = lambda row, half, blk=blk: blk(row, half, place.core)
        theirs = lambda row, half, blk=blk: blk(row, half, 1 - place.core)
        src = own if own is not None else (lambda half, mine=mine: mine(place.row, half))
        ring = Ring(place.row, place, place.in_col(1), place.in_col(-1), mine, src, ss.at[t], rs.at[t])
        out.append((ring, Pair(ring, place, theirs, cs.at[t], cr.at[t])))
    return out


def ring_start(ring, pair):
    ring.start()
    pair.give(0, 0, ring.own(0))
    pair.give(0, 1, ring.own(1))


def ring_finish(items):
    for ring, pair in items:
        ring.forward()
        pair.give(1, 0)
        pair.give(2, 1)
    for ring, pair in items:
        ring.rest()
        pair.give(1, 1)
        pair.give(2, 0)
    for ring, pair in items:
        ring.last()
        pair.give(3, 0)
        pair.give(3, 1)
    for ring, pair in items:
        pair.take()
    for ring, pair in items:
        ring.drain()
        pair.drain()


def weight_specs(wq, wu, wo, wd, wo_own, wd_own):
    cols = wq.shape[1] // 2
    o_rows, d_rows = wo.shape[2] // 2, wd.shape[2] // 2
    q_blk = lambda row, half, core: wq.at[row, pl.ds(half * cols, cols), core]
    u_blk = lambda row, half, core: wu.at[row, pl.ds(half * cols, cols), core]
    o_blk = lambda row, half, core: wo.at[row, core, pl.ds(half * o_rows, o_rows)]
    d_blk = lambda row, half, core: wd.at[row, core, pl.ds(half * d_rows, d_rows)]
    return [
        (d_blk, lambda half: wd_own.at[pl.ds(half * d_rows, d_rows)]),
        (o_blk, lambda half: wo_own.at[pl.ds(half * o_rows, o_rows)]),
        (q_blk, None),
        (u_blk, None),
    ]


def first_kernel(side, x_ref, small_ref, wq_ref, wu_ref, wo_ref, wd_ref,
                 small_all, xg, wq0, wu0, wo0, wd0, wq1s, wu1s,
                 sm_ss, sm_rs, x_ss, x_rs, a_ss, a_rs, w_ss, w_rs, c_ss, c_rs, loc):
    place = Place(side)
    count = side * side * CORES
    others = [lax.rem(place.me + d, count) for d in range(1, count)]
    meet(place, others)
    small_sent = []
    for d, dev in enumerate(others):
        small_sent.append(send(small_ref, small_all.at[place.me], sm_ss.at[d], sm_rs.at[d], dev))

    wide = wu_ref.shape[2] // (side * side)
    ex_sent = []

    def exchange(layer, q_dst, u_dst):
        for d in range(side):
            col = place.step(place.col, d)
            dev = place.in_row(d)
            q_src, u_at = wq_ref.at[layer, col], u_dst
            if d:
                ex_sent.append(send(q_src, q_dst, a_ss.at[layer, 0, d], a_rs.at[layer, 0, d], dev))
            else:
                pltpu.make_async_copy(q_src, q_dst, a_ss.at[layer, 0, d]).start()
            for k in range(side):
                off = pl.multiple_of((k * side + col) * wide, wide)
                src, dst = wu_ref.at[layer, :, pl.ds(off, wide)], u_at.at[:, pl.ds(k * wide, wide)]
                if d:
                    send(src, dst, a_ss.at[layer, 1, d], a_rs.at[layer, 1, d], dev)
                else:
                    pltpu.make_async_copy(src, dst, a_ss.at[layer, 1, d]).start()

    def exchanged(layer, kind, at):
        for d in range(side):
            dst = at(place.step(place.col, -d))
            arrived(dst, a_rs.at[layer, kind, d] if d else a_ss.at[layer, kind, d])

    exchange(0, wq0.at[place.row, place.col, place.core], wu0.at[place.row, place.col, place.core])

    items = weight_gather(place, weight_specs(wq0, wu0, wo0, wd0, wo_ref, wd_ref), (w_ss, w_rs, c_ss, c_rs))
    ring_start(*items[0])
    ring_start(*items[1])

    rows = x_ref.shape[0] // 2
    x_ring = Ring(place.col, place, place.in_row(1), place.in_row(-1), lambda col, half: xg.at[col, pl.ds(half * rows, rows)],
                  lambda half: x_ref.at[pl.ds(half * rows, rows)], x_ss, x_rs)
    x_ring.start()
    exchange(1, wq1s.at[place.col], wu1s.at[place.col])

    local = []
    for i, (src, dst) in enumerate(((small_ref, small_all.at[place.me]), (x_ref, xg.at[place.col]),
                                    (wo_ref, wo0.at[place.row, place.core]), (wd_ref, wd0.at[place.row, place.core]))):
        local.append(pltpu.make_async_copy(src, dst, loc.at[i]))
        local[-1].start()

    exchanged(0, 0, lambda col: wq0.at[place.row, col, place.core])
    ring_start(*items[2])
    exchanged(0, 1, lambda col: wu0.at[place.row, col, place.core])
    ring_start(*items[3])
    x_ring.forward()
    ring_finish(items)
    x_ring.rest()
    x_ring.last()
    x_ring.drain()
    exchanged(1, 0, lambda col: wq1s.at[col])
    exchanged(1, 1, lambda col: wu1s.at[col])
    for copy in ex_sent:
        copy.wait_send()
    for layer in range(2):
        for d in range(1, side):
            arrived(wu1s.at[0], a_ss.at[layer, 1, d])
    for d, dev in enumerate(others):
        src = lax.rem(place.me + count - d - 1, count)
        arrived(small_all.at[src], sm_rs.at[d])
        small_sent[d].wait_send()
    for copy in local:
        copy.wait()


def reduce_kernel(side, more, part_ref, x_ref, bias_ref, *refs):
    if more:
        (wq_own, wu_own, wo_ref, wd_ref, new_ref, xg, wq, wu, wo, wd,
         hop_a, hop_b, fin, r_ss, r_rs, x_ss, x_rs, w_ss, w_rs, c_ss, c_rs, loc) = refs
    else:
        new_ref, hop_a, hop_b, fin, r_ss, r_rs = refs
    place = Place(side)
    right, left = place.in_row(1), place.in_row(-1)
    devices = [right, left]
    if more:
        devices += [place.in_col(1), place.in_col(-1), place.sib]
    meet(place, devices)
    rows = part_ref.shape[1] // 2
    top, low = pl.ds(0, rows), pl.ds(rows, rows)
    nxt, prv, far = place.step(place.col, 1), place.step(place.col, -1), place.step(place.col, 2)
    sent = [
        send(part_ref.at[far, top], hop_a, r_ss.at[0], r_rs.at[0], left),
        send(part_ref.at[far, low], hop_b, r_ss.at[1], r_rs.at[1], right),
        send(part_ref.at[prv, low], fin.at[0], r_ss.at[2], r_rs.at[2], left),
        send(part_ref.at[nxt, top], fin.at[1], r_ss.at[3], r_rs.at[3], right),
    ]
    if more:
        q_rows = lambda ref: ref
        specs = weight_specs(wq, wu, wo, wd, wo_ref.at[1], wd_ref.at[1])
        cols = wq_own.shape[0] // 2
        specs[2] = (specs[2][0], lambda half: wq_own.at[pl.ds(half * cols, cols)])
        specs[3] = (specs[3][0], lambda half: wu_own.at[pl.ds(half * cols, cols)])
        items = weight_gather(place, specs, (w_ss, w_rs, c_ss, c_rs))
        for t in (2, 3, 1, 0):
            ring_start(*items[t])
        local = []
        for i, (src, dst) in enumerate(((wq_own, wq.at[place.row, :, place.core]), (wu_own, wu.at[place.row, :, place.core]),
                                        (wo_ref.at[1], wo.at[place.row, place.core]), (wd_ref.at[1], wd.at[place.row, place.core]))):
            local.append(pltpu.make_async_copy(src, dst, loc.at[i]))
            local[-1].start()

    tile = 16

    def add_into(hop, doc, first):
        @pl.loop(0, rows, step=tile)
        def _(r):
            hop[pl.ds(r, tile), :] = hop[pl.ds(r, tile), :] + part_ref[doc, pl.ds(first + r, tile), :]

    arrived(hop_a, r_rs.at[0])
    add_into(hop_a, prv, 0)
    sent.append(send(hop_a, fin.at[2], r_ss.at[4], r_rs.at[4], left))
    arrived(hop_b, r_rs.at[1])
    add_into(hop_b, nxt, rows)
    sent.append(send(hop_b, fin.at[3], r_ss.at[5], r_rs.at[5], right))
    for i in range(4):
        arrived(fin.at[i], r_rs.at[2 + i])

    def total(first, f_one, f_two):
        @pl.loop(0, rows, step=tile)
        def _(r):
            here, at = pl.ds(r, tile), pl.ds(first + r, tile)
            tot = part_ref[place.col, at, :] + fin[f_one, here, :] + fin[f_two, here, :]
            new_ref[at, :] = (x_ref[at, :].astype(jnp.float32) + (tot + bias_ref[...])).astype(jnp.bfloat16)

    total(0, 1, 2)
    total(rows, 0, 3)
    if more:
        x_ring = Ring(place.col, place, right, left, lambda col, half: xg.at[col, pl.ds(half * rows, rows)],
                      lambda half: new_ref.at[pl.ds(half * rows, rows)], x_ss, x_rs)
        x_ring.start()
        mine = pltpu.make_async_copy(new_ref, xg.at[place.col], loc.at[4])
        mine.start()
        x_ring.forward()
        x_ring.rest()
        x_ring.last()
        ring_finish([items[t] for t in (2, 3, 1, 0)])
        x_ring.drain()
        mine.wait()
        for copy in local:
            copy.wait()
    for copy in sent:
        copy.wait_send()


VM = pl.BlockSpec(memory_space=pltpu.VMEM)
ANY = pl.BlockSpec(memory_space=pl.ANY)
DMA = pltpu.SemaphoreType.DMA


def weight_shapes(side, wq_own, wu_own, wo, wd):
    bf = jnp.bfloat16
    return (
        jax.ShapeDtypeStruct((side, side, CORES) + wq_own, bf),
        jax.ShapeDtypeStruct((side, side, CORES) + wu_own, bf),
        jax.ShapeDtypeStruct((side, CORES) + wo, bf),
        jax.ShapeDtypeStruct((side, CORES) + wd, bf),
    )


WEIGHT_SEMS = [DMA((4, 6)), DMA((4, 6)), DMA((4, 8)), DMA((4, 8))]


def params(cid):
    return pltpu.CompilerParams(collective_id=cid, has_side_effects=True, vmem_limit_bytes=60 * 1024 * 1024)


def solution(mesh):
    row_spec = P(('dp', 'fsdp'), None, None)
    in_specs = (row_spec, P(('dp', 'fsdp')), P(None, None, 'fsdp'), P(None, 'fsdp', None, None), P(None, 'fsdp'), P(None, 'fsdp', None), P(None, 'fsdp'), P(None, 'fsdp', None), P(None, 'fsdp'), P(None, 'fsdp', None), P(None, 'fsdp'))
    count = mesh.shape['fsdp']
    side = math.isqrt(count // CORES)

    def local_step(hidden_loc, lens_loc, ln_par, w_qkv, b_qkv, w_out, b_out, w_up, b_up, w_down, b_down):
        layers = ln_par.shape[0]
        _, seq_len, d_model = hidden_loc.shape
        d_rows, heads, triple = w_qkv.shape[1:]
        head_dim = triple // 3
        per = heads // side
        ff = w_up.shape[2]
        bf, f32 = jnp.bfloat16, jnp.float32
        me = lax.axis_index('fsdp')
        core, col, row = me % CORES, (me // CORES) % side, me // (CORES * side)

        pieces = [ln_par, b_qkv, b_out, b_up, b_down, lens_loc]
        flat = jnp.concatenate([p.astype(f32).reshape(-1) for p in pieces])
        width = -(-flat.shape[0] // 1024) * 1024
        small = jnp.pad(flat, (0, width - flat.shape[0])).reshape(-1, 128)
        wq = w_qkv.reshape(layers, d_rows, per, side, triple).transpose(0, 3, 1, 2, 4).reshape(layers, side, d_rows, per * triple)
        x_own = hidden_loc[0]
        wq_own, wu_own = (d_rows, per * triple), (d_rows, ff // side)
        shapes = weight_shapes(side, wq_own, wu_own, w_out.shape[1:], w_down.shape[1:])

        outs = pl.pallas_call(
            functools.partial(first_kernel, side),
            out_shape=(
                jax.ShapeDtypeStruct((count,) + small.shape, f32),
                jax.ShapeDtypeStruct((side, seq_len, d_model), bf),
                *shapes,
                jax.ShapeDtypeStruct((side,) + wq_own, bf),
                jax.ShapeDtypeStruct((side,) + wu_own, bf),
            ),
            in_specs=[VM] * 6,
            out_specs=(ANY,) * 8,
            scratch_shapes=[DMA((count - 1,)), DMA((count - 1,)), DMA((6,)), DMA((6,)), DMA((2, 2, side)), DMA((2, 2, side)), *WEIGHT_SEMS, DMA((4,))],
            compiler_params=params(0),
        )(x_own, small, wq, w_up, w_out[0], w_down[0])
        small_all, xg, wq_x, wu_x, wo_x, wd_x, wq1s, wu1s = outs

        rows = small_all.reshape(count, width)
        got, at = [], 0
        for p in pieces:
            size = p.size
            part = rows[:, at:at + size].reshape((count,) + p.shape)
            got.append(jnp.moveaxis(part, 0, -2).reshape(p.shape[:-1] + (count * p.shape[-1],)))
            at += size
        ln_full, bq_full, bo_full, bu_full, bd_full, lens_full = got
        pick = lambda arr, axis: lax.dynamic_index_in_dim(arr, col, axis, keepdims=False)
        bq_x = pick(bq_full.reshape(layers, per, side, triple), 2).reshape(layers, per * triple)
        bu_x = pick(bu_full.reshape(layers, side, side, -1), 2).reshape(layers, ff // side)
        lens_grp = lax.dynamic_slice(lens_full.reshape(side, side, CORES), (row, 0, core), (1, side, 1)).reshape(side).astype(jnp.int32)
        bias = (bo_full + bd_full)[:, None, :]

        half = seq_len // 2
        rs_scratch = [pltpu.VMEM((half, d_model), f32), pltpu.VMEM((half, d_model), f32), pltpu.VMEM((4, half, d_model), f32), DMA((6,)), DMA((6,))]
        new_shape = jax.ShapeDtypeStruct((seq_len, d_model), bf)

        for layer in range(layers):
            flat2 = lambda w: w.reshape(-1, w.shape[-1])
            part = layer_partial(xg, lens_grp, ln_full[layer], flat2(wq_x), bq_x[layer], flat2(wo_x), flat2(wu_x), bu_x[layer], flat2(wd_x), head_dim)
            if layer == 0:
                x_own, xg, wq_x, wu_x, wo_x, wd_x = pl.pallas_call(
                    functools.partial(reduce_kernel, side, True),
                    out_shape=(new_shape, jax.ShapeDtypeStruct((side, seq_len, d_model), bf), *shapes),
                    in_specs=[VM] * 7,
                    out_specs=(VM,) + (ANY,) * 5,
                    scratch_shapes=[*rs_scratch, DMA((6,)), DMA((6,)), *WEIGHT_SEMS, DMA((5,))],
                    compiler_params=params(1),
                )(part, x_own, bias[layer], wq1s, wu1s, w_out, w_down)
            else:
                x_own = pl.pallas_call(
                    functools.partial(reduce_kernel, side, False),
                    out_shape=new_shape,
                    in_specs=[VM] * 3,
                    out_specs=VM,
                    scratch_shapes=rs_scratch,
                    compiler_params=params(2),
                )(part, x_own, bias[layer])
        return x_own[None]

    return jax.shard_map(local_step, mesh=mesh, in_specs=in_specs, out_specs=row_spec, check_vma=False)
```

```python
import functools
import math

import jax
import jax.numpy as jnp
import numpy as np
from jax import lax
from jax.experimental import pallas as pl
from jax.experimental.pallas import tpu as pltpu
from jax.sharding import PartitionSpec as P

ROPE_BASE = 10000.0
LN_EPS = 1e-5
CORES = 2
MESH = pl.DeviceIdType.MESH


def rotary_factors(seq_len, head_dim):
    rot = head_dim // 4
    half = rot // 2
    inv_freq = (1.0 / (ROPE_BASE ** (np.arange(0, rot, 2, dtype=np.float32) / rot))).astype(np.float32)
    angles = np.arange(seq_len, dtype=np.float32)[:, None] * inv_freq[None, :]
    cos, sin = np.cos(angles), np.sin(angles)
    out = np.zeros((3, seq_len, head_dim), np.float32)
    out[0] = 1.0
    out[0, :, :half], out[0, :, half:rot] = cos, cos
    out[1, :, :half] = -sin
    out[2, :, half:rot] = sin
    return jnp.asarray(out)


def send(src, dst, send_sem, recv_sem, dev):
    pltpu.make_async_remote_copy(src_ref=src, dst_ref=dst, send_sem=send_sem, recv_sem=recv_sem, device_id={"fsdp": dev}, device_id_type=MESH).start()


def settle(ref, sem):
    pltpu.make_async_copy(ref, ref, sem).wait()


class Place:
    def __init__(self, side):
        me = lax.axis_index("fsdp")
        self.side, self.me = side, me
        self.core = lax.rem(me, CORES)
        self.chip = me // CORES
        self.col = lax.rem(self.chip, side)
        self.row = self.chip // side
        self.sib = self.dev(self.row, self.col, 1 - self.core)

    def dev(self, row, col, core):
        return (row * self.side + col) * CORES + core

    def step(self, pos, by):
        return lax.rem(pos + by + self.side, self.side)

    def in_row(self, by):
        return self.dev(self.row, self.step(self.col, by), self.core)

    def in_col(self, by):
        return self.dev(self.step(self.row, by), self.col, self.core)


class Ring:
    def __init__(self, place, pos, right, left, blk, own, ss, rs):
        self.pos, self.right, self.left, self.blk, self.own, self.ss, self.rs = pos, right, left, blk, own, ss, rs
        self.prev, self.next, self.far = place.step(pos, -1), place.step(pos, 1), place.step(pos, 2)

    def _send(self, src, pos, half, i, j, dev):
        send(src, self.blk(pos, half), self.ss.at[i], self.rs.at[j], dev)

    def start(self):
        self._send(self.own(0), self.pos, 0, 0, 0, self.right)
        self._send(self.own(1), self.pos, 1, 2, 3, self.left)
        self._send(self.own(1), self.pos, 1, 1, 1, self.right)
        self._send(self.own(0), self.pos, 0, 3, 2, self.left)

    def forward(self):
        settle(self.blk(self.prev, 0), self.rs.at[0])
        self._send(self.blk(self.prev, 0), self.prev, 0, 4, 4, self.right)
        settle(self.blk(self.next, 1), self.rs.at[3])
        self._send(self.blk(self.next, 1), self.next, 1, 5, 5, self.left)

    def rest(self):
        settle(self.blk(self.prev, 1), self.rs.at[1])
        settle(self.blk(self.next, 0), self.rs.at[2])

    def last(self):
        settle(self.blk(self.far, 0), self.rs.at[4])
        settle(self.blk(self.far, 1), self.rs.at[5])

    def drain(self):
        for i, half in enumerate((0, 1, 1, 0, 0, 1)):
            settle(self.blk(self.pos, half), self.ss.at[i])


class Gather:
    def __init__(self, place, blk, own, ss, rs, cs, cr):
        mine = lambda row, half: blk(row, half, place.core)
        self.theirs = lambda row, half: blk(row, half, 1 - place.core)
        own = own if own is not None else (lambda half: mine(place.row, half))
        self.ring = Ring(place, place.row, place.in_col(1), place.in_col(-1), mine, own, ss, rs)
        self.sib, self.cs, self.cr = place.sib, cs, cr
        self.blocks = (self.ring.pos, self.ring.prev, self.ring.next, self.ring.far)

    def give(self, rel, half, src=None):
        i = rel * 2 + half
        blk = self.ring.blk(self.blocks[rel], half)
        send(blk if src is None else src, blk, self.cs.at[i], self.cr.at[i], self.sib)

    def start(self):
        self.ring.start()
        self.give(0, 0, self.ring.own(0))
        self.give(0, 1, self.ring.own(1))

    def forward(self):
        self.ring.forward()
        self.give(1, 0)
        self.give(2, 1)

    def finish(self):
        self.ring.rest()
        self.give(1, 1)
        self.give(2, 0)
        self.ring.last()
        self.give(3, 0)
        self.give(3, 1)
        for rel in range(4):
            for half in range(2):
                settle(self.theirs(self.blocks[rel], half), self.cr.at[rel * 2 + half])

    def drain(self):
        self.ring.drain()
        for rel in range(4):
            for half in range(2):
                settle(self.ring.blk(self.blocks[rel], half), self.cs.at[rel * 2 + half])


def weight_gathers(place, bufs, wo_own, wd_own, sems):
    wq, wu, wo, wd = bufs
    cols = wq.shape[1] // 2
    o_rows, d_rows = wo.shape[2] // 2, wd.shape[2] // 2
    specs = (
        (lambda row, half, core: wq.at[row, pl.ds(half * cols, cols), core], None),
        (lambda row, half, core: wu.at[row, pl.ds(half * cols, cols), core], None),
        (lambda row, half, core: wo.at[row, core, pl.ds(half * o_rows, o_rows)], lambda half: wo_own.at[pl.ds(half * o_rows, o_rows)]),
        (lambda row, half, core: wd.at[row, core, pl.ds(half * d_rows, d_rows)], lambda half: wd_own.at[pl.ds(half * d_rows, d_rows)]),
    )
    return [Gather(place, blk, own, *(s.at[t] for s in sems)) for t, (blk, own) in enumerate(specs)]


def both_layers(side, x_ref, vec_ref, bias_ref, rot_ref, wq_ref, wu_ref, wo_ref, wd_ref,
                out_ref, wq1, wu1, wo1, wd1,
                wq, wu, wo, wd, xg, xg1, a_buf, act, ctx, part, hop_a, hop_b, fin, vec_in, bias_in, vec, bq, bu,
                v_ss, v_rs, b_ss, b_rs, x_ss, x_rs, a_ss, a_rs, w_ss, w_rs, c_ss, c_rs, r_ss, r_rs, loc, loc1):
    f32, bf = jnp.float32, jnp.bfloat16
    place = Place(side)
    count = side * side * CORES
    seq, d_model = x_ref.shape
    head = rot_ref.shape[2]
    triple = 3 * head
    per = side
    ff = act.shape[2]
    half = seq // 2
    wide = wu_ref.shape[2] // (side * side)
    right, left = place.in_row(1), place.in_row(-1)
    nxt, prv, far = place.step(place.col, 1), place.step(place.col, -1), place.step(place.col, 2)

    barrier = pltpu.get_barrier_semaphore()
    others = [lax.rem(place.me + d, count) for d in range(1, count)]
    for dev in others:
        pl.semaphore_signal(barrier, inc=1, device_id={"fsdp": dev}, device_id_type=MESH)
    pl.semaphore_wait(barrier, count - 1)

    def exchange(layer, kind, dst_buf):
        for d in (1, 3, 2, 0):
            col = place.step(place.col, d)
            dst = dst_buf.at[place.row, place.col, place.core]
            pairs = [(wq_ref.at[layer, col], dst)]
            if kind:
                pairs = []
                for k in range(side):
                    off = pl.multiple_of((k * side + col) * wide, wide)
                    pairs.append((wu_ref.at[layer, :, pl.ds(off, wide)], dst.at[:, pl.ds(k * wide, wide)]))
            for src, to in pairs:
                if d:
                    send(src, to, a_ss.at[layer, kind, d], a_rs.at[layer, kind, d], place.in_row(d))
                else:
                    pltpu.make_async_copy(src, to, a_rs.at[layer, kind, d]).start()

    def exchanged(layer, kind, dst_buf):
        for d in range(side):
            settle(dst_buf.at[place.row, place.step(place.col, -d), place.core], a_rs.at[layer, kind, d])

    gathers = [
        weight_gathers(place, (wq, wu, wo, wd), wo_ref.at[0], wd_ref.at[0], [s.at[0] for s in (w_ss, w_rs, c_ss, c_rs)]),
        weight_gathers(place, (wq1, wu1, wo1, wd1), wo_ref.at[1], wd_ref.at[1], [s.at[1] for s in (w_ss, w_rs, c_ss, c_rs)]),
    ]
    gq, gu, go, gd = gathers[0]
    gq1, gu1, go1, gd1 = gathers[1]
    rows_of = lambda ref, col, h: ref.at[col, pl.ds(h * half, half)]
    x_ring = Ring(place, place.col, right, left, lambda col, h: rows_of(xg, col, h), lambda h: x_ref.at[pl.ds(h * half, half)], x_ss.at[0], x_rs.at[0])
    x1_ring = Ring(place, place.col, right, left, lambda col, h: rows_of(xg1, col, h), lambda h: rows_of(xg1, place.col, h), x_ss.at[1], x_rs.at[1])

    exchange(0, 0, wq)
    vec_at = lambda core, chip: vec_in.at[core, :, pl.ds(pl.multiple_of(chip * head, head), head)]
    bias_at = lambda core, row: bias_in.at[core, :, pl.ds(pl.multiple_of(row * head, head), head)]
    for d, dev in enumerate(others):
        send(vec_ref, vec_at(place.core, place.chip), v_ss.at[d], v_rs.at[d], dev)
    column = [(e, c) for e in range(side) for c in range(CORES) if e or c]
    for i, (e, c) in enumerate(column):
        dev = place.dev(place.step(place.row, e), place.col, lax.rem(place.core + c, CORES))
        send(bias_ref, bias_at(place.core, place.row), b_ss.at[i], b_rs.at[i], dev)
    exchange(0, 1, wu)
    go.start()
    x_ring.start()
    own = [(x_ref, xg.at[place.col]), (wo_ref.at[0], wo.at[place.row, place.core]), (wd_ref.at[0], wd.at[place.row, place.core]),
           (wo_ref.at[1], wo1.at[place.row, place.core]), (wd_ref.at[1], wd1.at[place.row, place.core])]
    for i, (src, dst) in enumerate(own):
        pltpu.make_async_copy(src, dst, loc.at[i]).start()

    vec_in[place.core, :, pl.ds(pl.multiple_of(place.chip * head, head), head)] = vec_ref[...]
    bias_in[place.core, :, pl.ds(pl.multiple_of(place.row * head, head), head)] = bias_ref[...]

    exchanged(0, 0, wq)
    gq.start()
    exchanged(0, 1, wu)
    gu.start()

    for d in range(1, count):
        src = lax.rem(place.me + count - d, count)
        settle(vec_at(lax.rem(src, CORES), src // CORES), v_rs.at[d - 1])
    for i, (e, c) in enumerate(column):
        settle(bias_at(lax.rem(place.core + c, CORES), place.step(place.row, -e)), b_rs.at[i])
    vec[...] = vec_in[0] + vec_in[1]
    for layer in range(2):
        for row in range(side):
            at = pl.ds(row * head, head)
            for t in range(3):
                i = layer * 3 + t
                bq[layer:layer + 1, row * triple + t * head:row * triple + (t + 1) * head] = bias_in[0, i:i + 1, at] + bias_in[1, i:i + 1, at]
            tiles = wide // head
            for t in range(tiles):
                i = 6 + layer * tiles + t
                bu[layer:layer + 1, row * wide + t * head:row * wide + (t + 1) * head] = bias_in[0, i:i + 1, at] + bias_in[1, i:i + 1, at]

    go.forward()
    x_ring.forward()
    exchange(1, 0, wq1)
    exchange(1, 1, wu1)
    gq.forward()
    gu.forward()
    gd.start()

    tile = min(32, half)

    def norm(src, doc, layer, which):
        gain, shift = vec[layer * 4 + which:layer * 4 + which + 1, :], vec[layer * 4 + which + 1:layer * 4 + which + 2, :]

        @pl.loop(0, seq, step=tile)
        def _(r):
            rows = src[doc, pl.ds(r, tile), :].astype(f32)
            centered = rows - jnp.mean(rows, axis=-1, keepdims=True)
            var = jnp.mean(centered * centered, axis=-1, keepdims=True)
            a_buf[pl.ds(r, tile), :] = (centered * lax.rsqrt(var + LN_EPS) * gain + shift).astype(bf)

    def attend(doc, layer):
        chip = place.row * side + doc
        lens = vec[12:13, pl.ds(pl.multiple_of(chip * head, head), head)]
        lane = lax.broadcasted_iota(jnp.int32, (1, head), 1)
        length = jnp.sum(jnp.where(lane == place.core * (head // CORES), lens, 0.0), axis=1, keepdims=True)
        query = lax.broadcasted_iota(jnp.int32, (seq, seq), 0)
        key = lax.broadcasted_iota(jnp.int32, (seq, seq), 1)
        visible = (key <= query) & (key.astype(f32) < length)
        pair = 2 * triple

        def turn(u):
            u = u.astype(f32)
            shift = head // 8
            return (u * rot_ref[0] + pltpu.roll(u, head - shift, 1) * rot_ref[1] + pltpu.roll(u, shift, 1) * rot_ref[2]).astype(bf)

        @pl.loop(0, per // 2)
        def _(p):
            at = pl.ds(pl.multiple_of(p * pair, pair), pair)
            w = wq[:, :, :, :, at].reshape(d_model, pair)
            qkv = (jnp.dot(a_buf[...], w, preferred_element_type=f32) + bq[layer:layer + 1, at]).astype(bf)
            for h in range(2):
                q, k, v = (qkv[:, h * triple + j * head:h * triple + (j + 1) * head] for j in range(3))
                scores = lax.dot_general(turn(q), turn(k), (((1,), (1,)), ((), ())), preferred_element_type=f32) * (head ** -0.5)
                scores = jnp.where(visible, scores, -1e30)
                probs = jnp.exp(scores - jnp.max(scores, axis=-1, keepdims=True))
                probs = (probs / jnp.sum(probs, axis=-1, keepdims=True)).astype(bf)
                to = pl.ds(pl.multiple_of((p * 2 + h) * head, head), head)
                ctx[doc, :, to] = jnp.dot(probs, v, preferred_element_type=f32).astype(bf)

    def up(doc, layer):
        step = ff // 4

        @pl.loop(0, 4)
        def _(n):
            at = pl.ds(pl.multiple_of(n * step, step), step)
            u = jnp.dot(a_buf[...], wu[:, :, :, :, at].reshape(d_model, step), preferred_element_type=f32) + bu[layer:layer + 1, at]
            act[doc, :, at] = (0.5 * u * (1.0 + lax.erf(u * (0.5 ** 0.5)))).astype(bf)

    def down(doc):
        step = d_model // 4

        @pl.loop(0, 4)
        def _(n):
            at = pl.ds(pl.multiple_of(n * step, step), step)
            tot = jnp.dot(ctx[doc], wo[:, :, :, at].reshape(per * head, step), preferred_element_type=f32)
            part[doc, :, at] = tot + jnp.dot(act[doc], wd[:, :, :, at].reshape(ff, step), preferred_element_type=f32)

    top, low = pl.ds(0, half), pl.ds(half, half)

    def send_far(layer):
        send(part.at[far, top], hop_a, r_ss.at[layer, 0], r_rs.at[layer, 0], left)
        send(part.at[far, low], hop_b, r_ss.at[layer, 1], r_rs.at[layer, 1], right)

    def send_prv(layer):
        send(part.at[prv, low], fin.at[0], r_ss.at[layer, 2], r_rs.at[layer, 2], left)

    def send_nxt(layer):
        send(part.at[nxt, top], fin.at[1], r_ss.at[layer, 3], r_rs.at[layer, 3], right)

    def pass_on(layer, i, hop, doc, first, dev):
        settle(hop, r_rs.at[layer, i])

        @pl.loop(0, half, step=tile)
        def _(r):
            hop[pl.ds(r, tile), :] = hop[pl.ds(r, tile), :] + part[doc, pl.ds(first + r, tile), :]

        send(hop, fin.at[2 + i], r_ss.at[layer, 4 + i], r_rs.at[layer, 4 + i], dev)

    def total(layer, src, first, f_one, f_two, store):
        @pl.loop(0, half, step=tile)
        def _(r):
            here, at = pl.ds(r, tile), pl.ds(first + r, tile)
            tot = part[place.col, at, :] + fin[f_one, here, :] + fin[f_two, here, :]
            bias = vec[8 + layer:9 + layer, :] + vec[10 + layer:11 + layer, :]
            store(at, (src[place.col, at, :].astype(f32) + (tot + bias)).astype(bf))

    def owner_sums(layer, src, store, done):
        for i in range(2, 6):
            settle(fin.at[0], r_rs.at[layer, i])
        total(layer, src, 0, 1, 2, store)
        total(layer, src, half, 0, 3, store)
        done()

    def sums_sent(layer):
        for i in range(6):
            settle(hop_a, r_ss.at[layer, i])

    settle(xg.at[place.col], loc.at[0])
    x_ring.rest()
    x_ring.last()
    gq.finish()

    @pl.loop(0, side)
    def _(doc):
        norm(xg, doc, 0, 0)
        attend(doc, 0)

    gu.finish()

    @pl.loop(0, side)
    def _(doc):
        norm(xg, doc, 0, 2)
        up(doc, 0)

        @pl.when(doc == 1)
        def _():
            gd.forward()

    go.finish()
    exchanged(1, 0, wq1)
    exchanged(1, 1, wu1)
    gq1.start()
    gu1.start()
    go1.start()
    gd1.start()
    settle(wo.at[place.row, place.core], loc.at[1])
    settle(wd.at[place.row, place.core], loc.at[2])
    gd.finish()

    @pl.loop(0, side)
    def _(i):
        doc = lax.rem(place.col + jnp.where(i == 0, 2, jnp.where(i == 1, 1, jnp.where(i == 2, side - 1, 0))), side)
        down(doc)

        @pl.when(i == 0)
        def _():
            send_far(0)

        @pl.when(i == 1)
        def _():
            send_nxt(0)

        @pl.when(i == 2)
        def _():
            send_prv(0)

    for g in gathers[0]:
        g.drain()
    gq1.forward()
    pass_on(0, 0, hop_a, prv, 0, left)
    pass_on(0, 1, hop_b, nxt, half, right)
    gu1.forward()
    go1.forward()

    def keep(at, rows):
        xg1[place.col, at, :] = rows

    owner_sums(0, xg, keep, x1_ring.start)
    gd1.forward()
    gq1.finish()
    load = [pltpu.make_async_copy(src, dst, loc1.at[i]) for i, (src, dst) in enumerate(((wq1, wq), (wu1, wu), (wo1, wo), (wd1, wd)))]
    load[0].start()
    sums_sent(0)
    load[0].wait()

    @pl.loop(0, side)
    def _(i):
        doc = lax.rem(place.col + jnp.where(i == 0, 0, jnp.where(i == 1, 1, jnp.where(i == 2, side - 1, 2))), side)

        @pl.when(i == 1)
        def _():
            x1_ring.rest()

        @pl.when(i == 3)
        def _():
            x1_ring.last()

        norm(xg1, doc, 1, 0)
        attend(doc, 1)

        @pl.when(i == 0)
        def _():
            x1_ring.forward()
            gu1.finish()
            pltpu.make_async_copy(wu1, wu, loc1.at[1]).start()
            go1.finish()
            settle(wo1.at[place.row, place.core], loc.at[3])
            pltpu.make_async_copy(wo1, wo, loc1.at[2]).start()
            settle(wu, loc1.at[1])

        norm(xg1, doc, 1, 2)
        up(doc, 1)

        @pl.when(i == 0)
        def _():
            settle(wd1.at[place.row, place.core], loc.at[4])
            gd1.finish()
            pltpu.make_async_copy(wd1, wd, loc1.at[3]).start()
            settle(wo, loc1.at[2])
            settle(wd, loc1.at[3])

        down(doc)

        @pl.when(i == 1)
        def _():
            send_nxt(1)

        @pl.when(i == 2)
        def _():
            send_prv(1)

        @pl.when(i == 3)
        def _():
            send_far(1)

    pass_on(1, 0, hop_a, prv, 0, left)
    pass_on(1, 1, hop_b, nxt, half, right)

    def give_out(at, rows):
        out_ref[at, :] = rows

    owner_sums(1, xg1, give_out, lambda: None)
    sums_sent(1)
    for g in gathers[1]:
        g.drain()
    x_ring.drain()
    x1_ring.drain()
    for d in range(count - 1):
        settle(vec_ref, v_ss.at[d])
    for i in range(len(column)):
        settle(bias_ref, b_ss.at[i])
    for layer in range(2):
        for kind, buf in enumerate((wq, wu)):
            for d in range(1, side):
                settle(buf.at[0, 0, 0], a_ss.at[layer, kind, d])


VM = pl.BlockSpec(memory_space=pltpu.VMEM)
ANY = pl.BlockSpec(memory_space=pl.ANY)
DMA = pltpu.SemaphoreType.DMA


def solution(mesh):
    row_spec = P(('dp', 'fsdp'), None, None)
    in_specs = (row_spec, P(('dp', 'fsdp')), P(None, None, 'fsdp'), P(None, 'fsdp', None, None), P(None, 'fsdp'), P(None, 'fsdp', None), P(None, 'fsdp'), P(None, 'fsdp', None), P(None, 'fsdp'), P(None, 'fsdp', None), P(None, 'fsdp'))
    count = mesh.shape['fsdp']
    side = math.isqrt(count // CORES)

    def local_step(hidden_loc, lens_loc, ln_par, w_qkv, b_qkv, w_out, b_out, w_up, b_up, w_down, b_down):
        layers = ln_par.shape[0]
        _, seq_len, d_model = hidden_loc.shape
        d_rows, heads, triple = w_qkv.shape[1:]
        head_dim = triple // 3
        per = heads // side
        ff_rows = w_down.shape[1]
        ff = ff_rows * CORES * side
        bf, f32 = jnp.bfloat16, jnp.float32
        core = lax.axis_index('fsdp') % CORES

        def placed(vals):
            zero = jnp.zeros_like(vals)
            return jnp.where(core == 0, jnp.concatenate([vals, zero], axis=-1), jnp.concatenate([zero, vals], axis=-1))

        lens_row = jnp.broadcast_to(lens_loc.astype(f32)[:, None], (1, d_rows))
        vec = jnp.concatenate([ln_par.reshape(-1, d_rows), b_out.astype(f32), b_down.astype(f32), lens_row, jnp.zeros((3, d_rows), f32)], axis=0)
        vec = placed(vec)
        bias = jnp.concatenate([placed(b_qkv.astype(f32)).reshape(-1, head_dim), placed(b_up.astype(f32)).reshape(-1, head_dim)], axis=0)
        bias = jnp.pad(bias, ((0, -bias.shape[0] % 16), (0, 0)))
        wq = w_qkv.reshape(layers, d_rows, per, side, triple).transpose(0, 3, 1, 2, 4).reshape(layers, side, d_rows, per * triple)

        half = seq_len // 2
        wq_s, wu_s = (side, side, CORES, d_rows, per * triple), (side, side, CORES, d_rows, ff)
        wo_s, wd_s = (side, CORES) + w_out.shape[1:], (side, CORES) + w_down.shape[1:]
        outs = pl.pallas_call(
            functools.partial(both_layers, side),
            out_shape=(jax.ShapeDtypeStruct((seq_len, d_model), bf), *(jax.ShapeDtypeStruct(s, bf) for s in (wq_s, wu_s, wo_s, wd_s))),
            in_specs=[ANY, VM, VM, VM, ANY, ANY, ANY, ANY],
            out_specs=(VM, ANY, ANY, ANY, ANY),
            scratch_shapes=[
                *(pltpu.VMEM(s, bf) for s in (wq_s, wu_s, wo_s, wd_s)),
                pltpu.VMEM((side, seq_len, d_model), bf),
                pltpu.VMEM((side, seq_len, d_model), bf),
                pltpu.VMEM((seq_len, d_model), bf),
                pltpu.VMEM((side, seq_len, ff), bf),
                pltpu.VMEM((side, seq_len, per * head_dim), bf),
                pltpu.VMEM((side, seq_len, d_model), f32),
                pltpu.VMEM((half, d_model), f32),
                pltpu.VMEM((half, d_model), f32),
                pltpu.VMEM((4, half, d_model), f32),
                pltpu.VMEM((CORES, 16, d_model), f32),
                pltpu.VMEM((CORES, bias.shape[0], side * head_dim), f32),
                pltpu.VMEM((16, d_model), f32),
                pltpu.VMEM((layers, per * triple), f32),
                pltpu.VMEM((layers, ff), f32),
                DMA((count - 1,)), DMA((count - 1,)), DMA((side * CORES - 1,)), DMA((side * CORES - 1,)),
                DMA((2, 6)), DMA((2, 6)), DMA((2, 2, side)), DMA((2, 2, side)),
                DMA((2, 4, 6)), DMA((2, 4, 6)), DMA((2, 4, 8)), DMA((2, 4, 8)),
                DMA((2, 6)), DMA((2, 6)), DMA((5,)), DMA((4,)),
            ],
            compiler_params=pltpu.CompilerParams(collective_id=0, has_side_effects=True, vmem_limit_bytes=67043328),
        )(hidden_loc[0], vec, bias, rotary_factors(seq_len, head_dim), wq, w_up, w_out, w_down)
        return outs[0][None]

    return jax.shard_map(local_step, mesh=mesh, in_specs=in_specs, out_specs=row_spec, check_vma=False)
```

```python
import functools
import math

import jax
import jax.numpy as jnp
import numpy as np
from jax import lax
from jax.experimental import pallas as pl
from jax.experimental.pallas import tpu as pltpu
from jax.sharding import PartitionSpec as P

ROPE_BASE = 10000.0
LN_EPS = 1e-5
CORES = 2
MESH = pl.DeviceIdType.MESH


def rotary_factors(seq_len, head_dim):
    rot = head_dim // 4
    half = rot // 2
    inv_freq = (1.0 / (ROPE_BASE ** (np.arange(0, rot, 2, dtype=np.float32) / rot))).astype(np.float32)
    angles = np.arange(seq_len, dtype=np.float32)[:, None] * inv_freq[None, :]
    cos, sin = np.cos(angles), np.sin(angles)
    out = np.zeros((3, seq_len, head_dim), np.float32)
    out[0] = 1.0
    out[0, :, :half], out[0, :, half:rot] = cos, cos
    out[1, :, :half] = -sin
    out[2, :, half:rot] = sin
    return jnp.asarray(out)


def send(src, dst, send_sem, recv_sem, dev):
    pltpu.make_async_remote_copy(src_ref=src, dst_ref=dst, send_sem=send_sem, recv_sem=recv_sem, device_id={"fsdp": dev}, device_id_type=MESH).start()


def settle(ref, sem):
    pltpu.make_async_copy(ref, ref, sem).wait()


class Place:
    def __init__(self, side):
        me = lax.axis_index("fsdp")
        self.side, self.me = side, me
        self.core = lax.rem(me, CORES)
        self.chip = me // CORES
        self.col = lax.rem(self.chip, side)
        self.row = self.chip // side
        self.sib = self.dev(self.row, self.col, 1 - self.core)

    def dev(self, row, col, core):
        return (row * self.side + col) * CORES + core

    def step(self, pos, by):
        return lax.rem(pos + by + self.side, self.side)

    def in_row(self, by):
        return self.dev(self.row, self.step(self.col, by), self.core)

    def in_col(self, by):
        return self.dev(self.step(self.row, by), self.col, self.core)


class Ring:
    def __init__(self, place, pos, right, left, blk, own, ss, rs):
        self.pos, self.right, self.left, self.blk, self.own, self.ss, self.rs = pos, right, left, blk, own, ss, rs
        self.prev, self.next, self.far = place.step(pos, -1), place.step(pos, 1), place.step(pos, 2)

    def _send(self, src, pos, half, i, j, dev):
        send(src, self.blk(pos, half), self.ss.at[i], self.rs.at[j], dev)

    def start(self):
        self._send(self.own(0), self.pos, 0, 0, 0, self.right)
        self._send(self.own(1), self.pos, 1, 2, 3, self.left)
        self._send(self.own(1), self.pos, 1, 1, 1, self.right)
        self._send(self.own(0), self.pos, 0, 3, 2, self.left)

    def forward(self):
        settle(self.blk(self.prev, 0), self.rs.at[0])
        self._send(self.blk(self.prev, 0), self.prev, 0, 4, 4, self.right)
        settle(self.blk(self.next, 1), self.rs.at[3])
        self._send(self.blk(self.next, 1), self.next, 1, 5, 5, self.left)

    def rest(self):
        settle(self.blk(self.prev, 1), self.rs.at[1])
        settle(self.blk(self.next, 0), self.rs.at[2])

    def last(self):
        settle(self.blk(self.far, 0), self.rs.at[4])
        settle(self.blk(self.far, 1), self.rs.at[5])

    def drain(self):
        for i, half in enumerate((0, 1, 1, 0, 0, 1)):
            settle(self.blk(self.pos, half), self.ss.at[i])


class Gather:
    def __init__(self, place, blk, own, ss, rs, cs, cr):
        mine = lambda row, half: blk(row, half, place.core)
        self.theirs = lambda row, half: blk(row, half, 1 - place.core)
        own = own if own is not None else (lambda half: mine(place.row, half))
        self.ring = Ring(place, place.row, place.in_col(1), place.in_col(-1), mine, own, ss, rs)
        self.sib, self.cs, self.cr = place.sib, cs, cr
        self.blocks = (self.ring.pos, self.ring.prev, self.ring.next, self.ring.far)

    def give(self, rel, half, src=None):
        i = rel * 2 + half
        blk = self.ring.blk(self.blocks[rel], half)
        send(blk if src is None else src, blk, self.cs.at[i], self.cr.at[i], self.sib)

    def start(self):
        self.ring.start()
        self.give(0, 0, self.ring.own(0))
        self.give(0, 1, self.ring.own(1))

    def forward(self):
        self.ring.forward()
        self.give(1, 0)
        self.give(2, 1)

    def finish(self):
        self.ring.rest()
        self.give(1, 1)
        self.give(2, 0)
        self.ring.last()
        self.give(3, 0)
        self.give(3, 1)
        for rel in range(4):
            for half in range(2):
                settle(self.theirs(self.blocks[rel], half), self.cr.at[rel * 2 + half])

    def drain(self):
        self.ring.drain()
        for rel in range(4):
            for half in range(2):
                settle(self.ring.blk(self.blocks[rel], half), self.cs.at[rel * 2 + half])


def weight_gathers(place, bufs, wo_own, wd_own, sems):
    wq, wu, wo, wd = bufs
    cols = wq.shape[1] // 2
    o_rows, d_rows, d_cols = wo.shape[2] // 2, wd.shape[3] // 2, wd.shape[4]
    specs = (
        (lambda row, half, core: wq.at[row, pl.ds(half * cols, cols), core], None),
        (lambda row, half, core: wu.at[row, pl.ds(half * cols, cols), core], None),
        (lambda row, half, core: wo.at[row, core, pl.ds(half * o_rows, o_rows)], lambda half: wo_own.at[pl.ds(half * o_rows, o_rows)]),
        *((lambda row, half, core, h=h: wd.at[h, row, core, pl.ds(half * d_rows, d_rows)],
           lambda half, h=h: wd_own.at[pl.ds(half * d_rows, d_rows), pl.ds(h * d_cols, d_cols)]) for h in range(2)),
    )
    return [Gather(place, blk, own, *(s.at[t] for s in sems)) for t, (blk, own) in enumerate(specs)]


def both_layers(side, x_ref, vec_ref, bias_ref, rot_ref, wq_ref, wu_ref, wo_ref, wd_ref,
                out_ref, wq1, wu1, wo1, wd1,
                wq, wu, wo, wd, xg, xg1, a_buf, act, ctx, part, hop_a, hop_b, fin, vec_in, bias_in, vec, bq, bu,
                v_ss, v_rs, b_ss, b_rs, x_ss, x_rs, a_ss, a_rs, w_ss, w_rs, c_ss, c_rs, r_ss, r_rs, loc, loc1):
    f32, bf = jnp.float32, jnp.bfloat16
    place = Place(side)
    count = side * side * CORES
    seq, d_model = x_ref.shape
    head = rot_ref.shape[2]
    triple = 3 * head
    per = side
    ff = act.shape[2]
    half = seq // 2
    wide = wu_ref.shape[2] // (side * side)
    right, left = place.in_row(1), place.in_row(-1)
    nxt, prv, far = place.step(place.col, 1), place.step(place.col, -1), place.step(place.col, 2)

    barrier = pltpu.get_barrier_semaphore()
    others = [lax.rem(place.me + d, count) for d in range(1, count)]
    for dev in others:
        pl.semaphore_signal(barrier, inc=1, device_id={"fsdp": dev}, device_id_type=MESH)
    pl.semaphore_wait(barrier, count - 1)

    def exchange(layer, kind, dst_buf):
        for d in (1, 3, 2, 0):
            col = place.step(place.col, d)
            dst = dst_buf.at[place.row, place.col, place.core]
            pairs = [(wq_ref.at[layer, col], dst)]
            if kind:
                pairs = []
                for k in range(side):
                    off = pl.multiple_of((k * side + col) * wide, wide)
                    pairs.append((wu_ref.at[layer, :, pl.ds(off, wide)], dst.at[:, pl.ds(k * wide, wide)]))
            for src, to in pairs:
                if d:
                    send(src, to, a_ss.at[layer, kind, d], a_rs.at[layer, kind, d], place.in_row(d))
                else:
                    pltpu.make_async_copy(src, to, a_rs.at[layer, kind, d]).start()

    def exchanged(layer, kind, dst_buf):
        for d in range(side):
            settle(dst_buf.at[place.row, place.step(place.col, -d), place.core], a_rs.at[layer, kind, d])

    gathers = [
        weight_gathers(place, (wq, wu, wo, wd), wo_ref.at[0], wd_ref.at[0], [s.at[0] for s in (w_ss, w_rs, c_ss, c_rs)]),
        weight_gathers(place, (wq1, wu1, wo1, wd1), wo_ref.at[1], wd_ref.at[1], [s.at[1] for s in (w_ss, w_rs, c_ss, c_rs)]),
    ]
    gq, gu, go, *gd = gathers[0]
    gq1, gu1, go1, *gd1 = gathers[1]
    d_cols = wd.shape[4]
    rows_of = lambda ref, col, h: ref.at[col, pl.ds(h * half, half)]
    x_ring = Ring(place, place.col, right, left, lambda col, h: rows_of(xg, col, h), lambda h: x_ref.at[pl.ds(h * half, half)], x_ss.at[0], x_rs.at[0])
    x1_ring = Ring(place, place.col, right, left, lambda col, h: rows_of(xg1, col, h), lambda h: rows_of(xg1, place.col, h), x_ss.at[1], x_rs.at[1])

    exchange(0, 0, wq)
    vec_at = lambda core, chip: vec_in.at[core, :, pl.ds(pl.multiple_of(chip * head, head), head)]
    bias_at = lambda core, row: bias_in.at[core, :, pl.ds(pl.multiple_of(row * head, head), head)]
    for d, dev in enumerate(others):
        send(vec_ref, vec_at(place.core, place.chip), v_ss.at[d], v_rs.at[d], dev)
    column = [(e, c) for e in range(side) for c in range(CORES) if e or c]
    for i, (e, c) in enumerate(column):
        dev = place.dev(place.step(place.row, e), place.col, lax.rem(place.core + c, CORES))
        send(bias_ref, bias_at(place.core, place.row), b_ss.at[i], b_rs.at[i], dev)
    exchange(0, 1, wu)
    go.start()
    gd[1].start()
    x_ring.start()
    own = [(x_ref, xg.at[place.col]), (wo_ref.at[0], wo.at[place.row, place.core]), (wo_ref.at[1], wo1.at[place.row, place.core])]
    own += [(wd_ref.at[layer, :, pl.ds(h * d_cols, d_cols)], buf.at[h, place.row, place.core]) for layer, buf in enumerate((wd, wd1)) for h in range(2)]
    for i, (src, dst) in enumerate(own):
        pltpu.make_async_copy(src, dst, loc.at[i]).start()

    vec_in[place.core, :, pl.ds(pl.multiple_of(place.chip * head, head), head)] = vec_ref[...]
    bias_in[place.core, :, pl.ds(pl.multiple_of(place.row * head, head), head)] = bias_ref[...]

    exchanged(0, 0, wq)
    gq.start()
    exchanged(0, 1, wu)
    gu.start()

    for d in range(1, count):
        src = lax.rem(place.me + count - d, count)
        settle(vec_at(lax.rem(src, CORES), src // CORES), v_rs.at[d - 1])
    for i, (e, c) in enumerate(column):
        settle(bias_at(lax.rem(place.core + c, CORES), place.step(place.row, -e)), b_rs.at[i])
    vec[...] = vec_in[0] + vec_in[1]
    for layer in range(2):
        for row in range(side):
            at = pl.ds(row * head, head)
            for t in range(3):
                i = layer * 3 + t
                bq[layer:layer + 1, row * triple + t * head:row * triple + (t + 1) * head] = bias_in[0, i:i + 1, at] + bias_in[1, i:i + 1, at]
            tiles = wide // head
            for t in range(tiles):
                i = 6 + layer * tiles + t
                bu[layer:layer + 1, row * wide + t * head:row * wide + (t + 1) * head] = bias_in[0, i:i + 1, at] + bias_in[1, i:i + 1, at]

    go.forward()
    x_ring.forward()
    exchange(1, 0, wq1)
    exchange(1, 1, wu1)
    gq.forward()
    gu.forward()
    gd[0].start()

    tile = min(32, half)

    def norm(src, doc, layer, which):
        gain, shift = vec[layer * 4 + which:layer * 4 + which + 1, :], vec[layer * 4 + which + 1:layer * 4 + which + 2, :]

        @pl.loop(0, seq, step=tile)
        def _(r):
            rows = src[doc, pl.ds(r, tile), :].astype(f32)
            centered = rows - jnp.mean(rows, axis=-1, keepdims=True)
            var = jnp.mean(centered * centered, axis=-1, keepdims=True)
            a_buf[pl.ds(r, tile), :] = (centered * lax.rsqrt(var + LN_EPS) * gain + shift).astype(bf)

    def attend(doc, layer):
        chip = place.row * side + doc
        lens = vec[12:13, pl.ds(pl.multiple_of(chip * head, head), head)]
        lane = lax.broadcasted_iota(jnp.int32, (1, head), 1)
        length = jnp.sum(jnp.where(lane == place.core * (head // CORES), lens, 0.0), axis=1, keepdims=True)
        query = lax.broadcasted_iota(jnp.int32, (seq, seq), 0)
        key = lax.broadcasted_iota(jnp.int32, (seq, seq), 1)
        visible = (key <= query) & (key.astype(f32) < length)
        pair = 2 * triple

        def turn(u):
            u = u.astype(f32)
            shift = head // 8
            return (u * rot_ref[0] + pltpu.roll(u, head - shift, 1) * rot_ref[1] + pltpu.roll(u, shift, 1) * rot_ref[2]).astype(bf)

        @pl.loop(0, per // 2)
        def _(p):
            at = pl.ds(pl.multiple_of(p * pair, pair), pair)
            w = wq[:, :, :, :, at].reshape(d_model, pair)
            qkv = (jnp.dot(a_buf[...], w, preferred_element_type=f32) + bq[layer:layer + 1, at]).astype(bf)
            for h in range(2):
                q, k, v = (qkv[:, h * triple + j * head:h * triple + (j + 1) * head] for j in range(3))
                scores = lax.dot_general(turn(q), turn(k), (((1,), (1,)), ((), ())), preferred_element_type=f32) * (head ** -0.5)
                scores = jnp.where(visible, scores, -1e30)
                probs = jnp.exp(scores - jnp.max(scores, axis=-1, keepdims=True))
                probs = (probs / jnp.sum(probs, axis=-1, keepdims=True)).astype(bf)
                to = pl.ds(pl.multiple_of((p * 2 + h) * head, head), head)
                ctx[doc, :, to] = jnp.dot(probs, v, preferred_element_type=f32).astype(bf)

    def up(doc, layer):
        step = ff // 4

        @pl.loop(0, 4)
        def _(n):
            at = pl.ds(pl.multiple_of(n * step, step), step)
            u = jnp.dot(a_buf[...], wu[:, :, :, :, at].reshape(d_model, step), preferred_element_type=f32) + bu[layer:layer + 1, at]
            act[doc, :, at] = (0.5 * u * (1.0 + lax.erf(u * (0.5 ** 0.5)))).astype(bf)

    def down(doc, h):
        step = d_cols // 2

        @pl.loop(0, 2)
        def _(n):
            at = pl.ds(pl.multiple_of(n * step, step), step)
            wide_at = pl.ds(pl.multiple_of(h * d_cols + n * step, step), step)
            tot = jnp.dot(ctx[doc], wo[:, :, :, wide_at].reshape(per * head, step), preferred_element_type=f32)
            part[doc, h, :, at] = tot + jnp.dot(act[doc], wd[h, :, :, :, at].reshape(ff, step), preferred_element_type=f32)

    top, low = pl.ds(0, half), pl.ds(half, half)

    def send_far(layer, h):
        send(part.at[far, h, top], hop_a.at[h], r_ss.at[layer, h, 0], r_rs.at[layer, h, 0], left)
        send(part.at[far, h, low], hop_b.at[h], r_ss.at[layer, h, 1], r_rs.at[layer, h, 1], right)

    def send_prv(layer, h):
        send(part.at[prv, h, low], fin.at[0, h], r_ss.at[layer, h, 2], r_rs.at[layer, h, 2], left)

    def send_nxt(layer, h):
        send(part.at[nxt, h, top], fin.at[1, h], r_ss.at[layer, h, 3], r_rs.at[layer, h, 3], right)

    def pass_on(layer, h):
        for i, hop, doc, first, dev in ((0, hop_a, prv, 0, left), (1, hop_b, nxt, half, right)):
            settle(hop.at[h], r_rs.at[layer, h, i])

            @pl.loop(0, half, step=tile)
            def _(r, hop=hop, doc=doc, first=first):
                hop[h, pl.ds(r, tile), :] = hop[h, pl.ds(r, tile), :] + part[doc, h, pl.ds(first + r, tile), :]

            send(hop.at[h], fin.at[2 + i, h], r_ss.at[layer, h, 4 + i], r_rs.at[layer, h, 4 + i], dev)

    def owner_sums(layer, src, store):
        for h in range(2):
            cols = slice(h * d_cols, (h + 1) * d_cols)
            for i in range(2, 6):
                settle(fin.at[i - 2, h], r_rs.at[layer, h, i])
            for first, f_one, f_two in ((0, 1, 2), (half, 0, 3)):
                @pl.loop(0, half, step=tile)
                def _(r, first=first, f_one=f_one, f_two=f_two):
                    here, at = pl.ds(r, tile), pl.ds(first + r, tile)
                    tot = part[place.col, h, at, :] + fin[f_one, h, here, :] + fin[f_two, h, here, :]
                    bias = vec[8 + layer:9 + layer, cols] + vec[10 + layer:11 + layer, cols]
                    store(at, cols, (src[place.col, at, cols].astype(f32) + (tot + bias)).astype(bf))

    def sums_sent(layer):
        for h in range(2):
            for i in range(6):
                settle(hop_a.at[h], r_ss.at[layer, h, i])

    settle(xg.at[place.col], loc.at[0])
    x_ring.rest()
    x_ring.last()
    gq.finish()

    @pl.loop(0, side)
    def _(doc):
        norm(xg, doc, 0, 0)
        attend(doc, 0)

    gu.finish()

    @pl.loop(0, side)
    def _(doc):
        norm(xg, doc, 0, 2)
        up(doc, 0)

        @pl.when(doc == 1)
        def _():
            gd[0].forward()

    gd[1].forward()
    go.finish()
    settle(wo.at[place.row, place.core], loc.at[1])
    exchanged(1, 0, wq1)
    exchanged(1, 1, wu1)
    gq1.start()
    gu1.start()

    for h in range(2):
        settle(wd.at[h, place.row, place.core], loc.at[3 + h])
        gd[h].finish()

        @pl.loop(0, side)
        def _(i, h=h):
            doc = lax.rem(place.col + jnp.where(i == 0, 2, jnp.where(i == 1, 1, jnp.where(i == 2, side - 1, 0))), side)
            down(doc, h)

            @pl.when(i == 0)
            def _():
                send_far(0, h)

            @pl.when(i == 1)
            def _():
                send_nxt(0, h)

            @pl.when(i == 2)
            def _():
                send_prv(0, h)

    gq1.forward()
    pass_on(0, 0)
    pass_on(0, 1)
    gu1.forward()
    go1.start()
    gd1[0].start()
    gd1[1].start()
    for g in gathers[0]:
        g.drain()
    gq1.finish()
    pltpu.make_async_copy(wq1, wq, loc1.at[0]).start()
    gu1.finish()
    pltpu.make_async_copy(wu1, wu, loc1.at[1]).start()

    def keep(at, cols, rows):
        xg1[place.col, at, cols] = rows

    owner_sums(0, xg, keep)
    x1_ring.start()
    go1.forward()
    sums_sent(0)
    settle(wq, loc1.at[0])
    settle(wu, loc1.at[1])

    @pl.loop(0, side)
    def _(i):
        doc = lax.rem(place.col + jnp.where(i == 0, 0, jnp.where(i == 1, 1, jnp.where(i == 2, side - 1, 2))), side)

        @pl.when(i == 1)
        def _():
            x1_ring.rest()

        @pl.when(i == 2)
        def _():
            settle(wo1.at[place.row, place.core], loc.at[2])
            go1.finish()
            pltpu.make_async_copy(wo1, wo, loc1.at[2]).start()
            settle(wd1.at[0, place.row, place.core], loc.at[5])
            gd1[0].finish()
            pltpu.make_async_copy(wd1.at[0], wd.at[0], loc1.at[3]).start()

        @pl.when(i == 3)
        def _():
            x1_ring.last()

        norm(xg1, doc, 1, 0)
        attend(doc, 1)
        norm(xg1, doc, 1, 2)
        up(doc, 1)

        @pl.when(i == 0)
        def _():
            x1_ring.forward()
            gd1[0].forward()
            gd1[1].forward()

        @pl.when(i == 2)
        def _():
            settle(wd1.at[1, place.row, place.core], loc.at[6])
            gd1[1].finish()
            pltpu.make_async_copy(wd1.at[1], wd.at[1], loc1.at[4]).start()
            settle(wo, loc1.at[2])
            settle(wd.at[0], loc1.at[3])
            down(nxt, 0)
            send_nxt(1, 0)
            down(prv, 0)
            send_prv(1, 0)
            settle(wd.at[1], loc1.at[4])
            down(nxt, 1)
            send_nxt(1, 1)
            down(prv, 1)
            send_prv(1, 1)

        @pl.when(i == 3)
        def _():
            for h in range(2):
                down(far, h)
                send_far(1, h)
            for h in range(2):
                down(place.col, h)

    pass_on(1, 0)
    pass_on(1, 1)

    def give_out(at, cols, rows):
        out_ref[at, cols] = rows

    owner_sums(1, xg1, give_out)
    sums_sent(1)
    for g in gathers[1]:
        g.drain()
    x_ring.drain()
    x1_ring.drain()
    for d in range(count - 1):
        settle(vec_ref, v_ss.at[d])
    for i in range(len(column)):
        settle(bias_ref, b_ss.at[i])
    for layer in range(2):
        for kind, buf in enumerate((wq, wu)):
            for d in range(1, side):
                settle(buf.at[0, 0, 0], a_ss.at[layer, kind, d])


VM = pl.BlockSpec(memory_space=pltpu.VMEM)
ANY = pl.BlockSpec(memory_space=pl.ANY)
DMA = pltpu.SemaphoreType.DMA


def solution(mesh):
    row_spec = P(('dp', 'fsdp'), None, None)
    in_specs = (row_spec, P(('dp', 'fsdp')), P(None, None, 'fsdp'), P(None, 'fsdp', None, None), P(None, 'fsdp'), P(None, 'fsdp', None), P(None, 'fsdp'), P(None, 'fsdp', None), P(None, 'fsdp'), P(None, 'fsdp', None), P(None, 'fsdp'))
    count = mesh.shape['fsdp']
    side = math.isqrt(count // CORES)

    def local_step(hidden_loc, lens_loc, ln_par, w_qkv, b_qkv, w_out, b_out, w_up, b_up, w_down, b_down):
        layers = ln_par.shape[0]
        _, seq_len, d_model = hidden_loc.shape
        d_rows, heads, triple = w_qkv.shape[1:]
        head_dim = triple // 3
        per = heads // side
        ff_rows = w_down.shape[1]
        ff = ff_rows * CORES * side
        bf, f32 = jnp.bfloat16, jnp.float32
        core = lax.axis_index('fsdp') % CORES

        def placed(vals):
            zero = jnp.zeros_like(vals)
            return jnp.where(core == 0, jnp.concatenate([vals, zero], axis=-1), jnp.concatenate([zero, vals], axis=-1))

        lens_row = jnp.broadcast_to(lens_loc.astype(f32)[:, None], (1, d_rows))
        vec = jnp.concatenate([ln_par.reshape(-1, d_rows), b_out.astype(f32), b_down.astype(f32), lens_row, jnp.zeros((3, d_rows), f32)], axis=0)
        vec = placed(vec)
        bias = jnp.concatenate([placed(b_qkv.astype(f32)).reshape(-1, head_dim), placed(b_up.astype(f32)).reshape(-1, head_dim)], axis=0)
        bias = jnp.pad(bias, ((0, -bias.shape[0] % 16), (0, 0)))
        wq = w_qkv.reshape(layers, d_rows, per, side, triple).transpose(0, 3, 1, 2, 4).reshape(layers, side, d_rows, per * triple)

        half = seq_len // 2
        wq_s, wu_s = (side, side, CORES, d_rows, per * triple), (side, side, CORES, d_rows, ff)
        wo_s, wd_s = (side, CORES) + w_out.shape[1:], (2, side, CORES, ff_rows, d_model // 2)
        outs = pl.pallas_call(
            functools.partial(both_layers, side),
            out_shape=(jax.ShapeDtypeStruct((seq_len, d_model), bf), *(jax.ShapeDtypeStruct(s, bf) for s in (wq_s, wu_s, wo_s, wd_s))),
            in_specs=[ANY, VM, VM, VM, ANY, ANY, ANY, ANY],
            out_specs=(VM, ANY, ANY, ANY, ANY),
            scratch_shapes=[
                *(pltpu.VMEM(s, bf) for s in (wq_s, wu_s, wo_s, wd_s)),
                pltpu.VMEM((side, seq_len, d_model), bf),
                pltpu.VMEM((side, seq_len, d_model), bf),
                pltpu.VMEM((seq_len, d_model), bf),
                pltpu.VMEM((side, seq_len, ff), bf),
                pltpu.VMEM((side, seq_len, per * head_dim), bf),
                pltpu.VMEM((side, 2, seq_len, d_model // 2), f32),
                pltpu.VMEM((2, half, d_model // 2), f32),
                pltpu.VMEM((2, half, d_model // 2), f32),
                pltpu.VMEM((4, 2, half, d_model // 2), f32),
                pltpu.VMEM((CORES, 16, d_model), f32),
                pltpu.VMEM((CORES, bias.shape[0], side * head_dim), f32),
                pltpu.VMEM((16, d_model), f32),
                pltpu.VMEM((layers, per * triple), f32),
                pltpu.VMEM((layers, ff), f32),
                DMA((count - 1,)), DMA((count - 1,)), DMA((side * CORES - 1,)), DMA((side * CORES - 1,)),
                DMA((2, 6)), DMA((2, 6)), DMA((2, 2, side)), DMA((2, 2, side)),
                DMA((2, 5, 6)), DMA((2, 5, 6)), DMA((2, 5, 8)), DMA((2, 5, 8)),
                DMA((2, 2, 6)), DMA((2, 2, 6)), DMA((7,)), DMA((5,)),
            ],
            compiler_params=pltpu.CompilerParams(collective_id=0, has_side_effects=True, vmem_limit_bytes=67043328),
        )(hidden_loc[0], vec, bias, rotary_factors(seq_len, head_dim), wq, w_up, w_out, w_down)
        return outs[0][None]

    return jax.shard_map(local_step, mesh=mesh, in_specs=in_specs, out_specs=row_spec, check_vma=False)
```

```python
import functools
import math

import jax
import jax.numpy as jnp
import numpy as np
from jax import lax
from jax.experimental import pallas as pl
from jax.experimental.pallas import tpu as pltpu
from jax.sharding import PartitionSpec as P

ROPE_BASE = 10000.0
LN_EPS = 1e-5
CORES = 2
MESH = pl.DeviceIdType.MESH


def rotary_factors(seq_len, head_dim):
    rot = head_dim // 4
    half = rot // 2
    inv_freq = (1.0 / (ROPE_BASE ** (np.arange(0, rot, 2, dtype=np.float32) / rot))).astype(np.float32)
    angles = np.arange(seq_len, dtype=np.float32)[:, None] * inv_freq[None, :]
    cos, sin = np.cos(angles), np.sin(angles)
    out = np.zeros((3, seq_len, head_dim), np.float32)
    out[0] = 1.0
    out[0, :, :half], out[0, :, half:rot] = cos, cos
    out[1, :, :half] = -sin
    out[2, :, half:rot] = sin
    return jnp.asarray(out)


def send(src, dst, send_sem, recv_sem, dev):
    pltpu.make_async_remote_copy(src_ref=src, dst_ref=dst, send_sem=send_sem, recv_sem=recv_sem, device_id={"fsdp": dev}, device_id_type=MESH).start()


def settle(ref, sem):
    pltpu.make_async_copy(ref, ref, sem).wait()


class Place:
    def __init__(self, side):
        me = lax.axis_index("fsdp")
        self.side, self.me = side, me
        self.core = lax.rem(me, CORES)
        self.chip = me // CORES
        self.col = lax.rem(self.chip, side)
        self.row = self.chip // side
        self.sib = self.dev(self.row, self.col, 1 - self.core)

    def dev(self, row, col, core):
        return (row * self.side + col) * CORES + core

    def step(self, pos, by):
        return lax.rem(pos + by + self.side, self.side)

    def in_row(self, by):
        return self.dev(self.row, self.step(self.col, by), self.core)

    def in_col(self, by):
        return self.dev(self.step(self.row, by), self.col, self.core)


class Ring:
    def __init__(self, place, pos, right, left, blk, own, ss, rs):
        self.pos, self.right, self.left, self.blk, self.own, self.ss, self.rs = pos, right, left, blk, own, ss, rs
        self.prev, self.next, self.far = place.step(pos, -1), place.step(pos, 1), place.step(pos, 2)

    def _send(self, src, pos, half, i, j, dev):
        send(src, self.blk(pos, half), self.ss.at[i], self.rs.at[j], dev)

    def start(self):
        self._send(self.own(0), self.pos, 0, 0, 0, self.right)
        self._send(self.own(1), self.pos, 1, 2, 3, self.left)
        self._send(self.own(1), self.pos, 1, 1, 1, self.right)
        self._send(self.own(0), self.pos, 0, 3, 2, self.left)

    def forward(self):
        settle(self.blk(self.prev, 0), self.rs.at[0])
        self._send(self.blk(self.prev, 0), self.prev, 0, 4, 4, self.right)
        settle(self.blk(self.next, 1), self.rs.at[3])
        self._send(self.blk(self.next, 1), self.next, 1, 5, 5, self.left)

    def rest(self):
        settle(self.blk(self.prev, 1), self.rs.at[1])
        settle(self.blk(self.next, 0), self.rs.at[2])

    def last(self):
        settle(self.blk(self.far, 0), self.rs.at[4])
        settle(self.blk(self.far, 1), self.rs.at[5])

    def drain(self):
        for i, half in enumerate((0, 1, 1, 0, 0, 1)):
            settle(self.blk(self.pos, half), self.ss.at[i])


class Gather:
    def __init__(self, place, blk, own, ss, rs, cs, cr):
        mine = lambda row, half: blk(row, half, place.core)
        self.theirs = lambda row, half: blk(row, half, 1 - place.core)
        own = own if own is not None else (lambda half: mine(place.row, half))
        self.ring = Ring(place, place.row, place.in_col(1), place.in_col(-1), mine, own, ss, rs)
        self.sib, self.cs, self.cr = place.sib, cs, cr
        self.blocks = (self.ring.pos, self.ring.prev, self.ring.next, self.ring.far)

    def give(self, rel, half, src=None):
        i = rel * 2 + half
        blk = self.ring.blk(self.blocks[rel], half)
        send(blk if src is None else src, blk, self.cs.at[i], self.cr.at[i], self.sib)

    def start(self):
        self.ring.start()
        self.give(0, 0, self.ring.own(0))
        self.give(0, 1, self.ring.own(1))

    def forward(self):
        self.ring.forward()
        self.give(1, 0)
        self.give(2, 1)

    def finish(self):
        self.ring.rest()
        self.give(1, 1)
        self.give(2, 0)
        self.ring.last()
        self.give(3, 0)
        self.give(3, 1)
        for rel in range(4):
            for half in range(2):
                settle(self.theirs(self.blocks[rel], half), self.cr.at[rel * 2 + half])

    def drain(self):
        self.ring.drain()
        for rel in range(4):
            for half in range(2):
                settle(self.ring.blk(self.blocks[rel], half), self.cs.at[rel * 2 + half])


def weight_gathers(place, bufs, wo_own, wd_own, sems):
    wq, wu, wo, wd = bufs
    cols = wq.shape[1] // 2
    o_rows, d_rows, d_cols = wo.shape[2] // 2, wd.shape[3] // 2, wd.shape[4]
    specs = (
        (lambda row, half, core: wq.at[row, pl.ds(half * cols, cols), core], None),
        (lambda row, half, core: wu.at[row, pl.ds(half * cols, cols), core], None),
        (lambda row, half, core: wo.at[row, core, pl.ds(half * o_rows, o_rows)], lambda half: wo_own.at[pl.ds(half * o_rows, o_rows)]),
        *((lambda row, half, core, h=h: wd.at[h, row, core, pl.ds(half * d_rows, d_rows)],
           lambda half, h=h: wd_own.at[pl.ds(half * d_rows, d_rows), pl.ds(h * d_cols, d_cols)]) for h in range(2)),
    )
    return [Gather(place, blk, own, *(s.at[t] for s in sems)) for t, (blk, own) in enumerate(specs)]


def both_layers(side, x_ref, vec_ref, bias_ref, rot_ref, wq_ref, wu_ref, wo_ref, wd_ref,
                out_ref, wq1, wu1, wo1, wd1,
                wq, wu, wo, wd, xg, xg1, a_buf, m_buf, act, ctx, part, hop_a, hop_b, fin, vec_in, bias_in, vec, bq, bu,
                v_ss, v_rs, b_ss, b_rs, x_ss, x_rs, a_ss, a_rs, w_ss, w_rs, c_ss, c_rs, r_ss, r_rs, loc, loc1):
    f32, bf = jnp.float32, jnp.bfloat16
    place = Place(side)
    count = side * side * CORES
    seq, d_model = x_ref.shape
    head = rot_ref.shape[2]
    triple = 3 * head
    per = side
    ff = act.shape[2]
    half = seq // 2
    wide = wu_ref.shape[2] // (side * side)
    right, left = place.in_row(1), place.in_row(-1)
    nxt, prv, far = place.step(place.col, 1), place.step(place.col, -1), place.step(place.col, 2)

    barrier = pltpu.get_barrier_semaphore()
    others = [lax.rem(place.me + d, count) for d in range(1, count)]
    for dev in others:
        pl.semaphore_signal(barrier, inc=1, device_id={"fsdp": dev}, device_id_type=MESH)
    pl.semaphore_wait(barrier, count - 1)

    def exchange(layer, kind, dst_buf):
        for d in (1, 3, 2, 0):
            col = place.step(place.col, d)
            dst = dst_buf.at[place.row, place.col, place.core]
            pairs = [(wq_ref.at[layer, col], dst)]
            if kind:
                pairs = []
                for k in range(side):
                    off = pl.multiple_of((k * side + col) * wide, wide)
                    pairs.append((wu_ref.at[layer, :, pl.ds(off, wide)], dst.at[:, pl.ds(k * wide, wide)]))
            for src, to in pairs:
                if d:
                    send(src, to, a_ss.at[layer, kind, d], a_rs.at[layer, kind, d], place.in_row(d))
                else:
                    pltpu.make_async_copy(src, to, a_rs.at[layer, kind, d]).start()

    def exchanged(layer, kind, dst_buf):
        for d in range(side):
            settle(dst_buf.at[place.row, place.step(place.col, -d), place.core], a_rs.at[layer, kind, d])

    gathers = [
        weight_gathers(place, (wq, wu, wo, wd), wo_ref.at[0], wd_ref.at[0], [s.at[0] for s in (w_ss, w_rs, c_ss, c_rs)]),
        weight_gathers(place, (wq1, wu1, wo1, wd1), wo_ref.at[1], wd_ref.at[1], [s.at[1] for s in (w_ss, w_rs, c_ss, c_rs)]),
    ]
    gq, gu, go, *gd = gathers[0]
    gq1, gu1, go1, *gd1 = gathers[1]
    d_cols = wd.shape[4]
    rows_of = lambda ref, col, h: ref.at[col, pl.ds(h * half, half)]
    x_ring = Ring(place, place.col, right, left, lambda col, h: rows_of(xg, col, h), lambda h: x_ref.at[pl.ds(h * half, half)], x_ss.at[0], x_rs.at[0])
    x1_ring = Ring(place, place.col, right, left, lambda col, h: rows_of(xg1, col, h), lambda h: rows_of(xg1, place.col, h), x_ss.at[1], x_rs.at[1])

    exchange(0, 0, wq)
    vec_at = lambda core, chip: vec_in.at[core, :, pl.ds(pl.multiple_of(chip * head, head), head)]
    bias_at = lambda core, row: bias_in.at[core, :, pl.ds(pl.multiple_of(row * head, head), head)]
    for d, dev in enumerate(others):
        send(vec_ref, vec_at(place.core, place.chip), v_ss.at[d], v_rs.at[d], dev)
    column = [(e, c) for e in range(side) for c in range(CORES) if e or c]
    for i, (e, c) in enumerate(column):
        dev = place.dev(place.step(place.row, e), place.col, lax.rem(place.core + c, CORES))
        send(bias_ref, bias_at(place.core, place.row), b_ss.at[i], b_rs.at[i], dev)
    exchange(0, 1, wu)
    go.start()
    gd[1].start()
    x_ring.start()
    own = [(x_ref, xg.at[place.col]), (wo_ref.at[0], wo.at[place.row, place.core]), (wo_ref.at[1], wo1.at[place.row, place.core])]
    own += [(wd_ref.at[layer, :, pl.ds(h * d_cols, d_cols)], buf.at[h, place.row, place.core]) for layer, buf in enumerate((wd, wd1)) for h in range(2)]
    for i, (src, dst) in enumerate(own):
        pltpu.make_async_copy(src, dst, loc.at[i]).start()

    vec_in[place.core, :, pl.ds(pl.multiple_of(place.chip * head, head), head)] = vec_ref[...]
    bias_in[place.core, :, pl.ds(pl.multiple_of(place.row * head, head), head)] = bias_ref[...]

    exchanged(0, 0, wq)
    gq.start()
    exchanged(0, 1, wu)
    gq.forward()
    gu.start()

    for d in range(1, count):
        src = lax.rem(place.me + count - d, count)
        settle(vec_at(lax.rem(src, CORES), src // CORES), v_rs.at[d - 1])
    for i, (e, c) in enumerate(column):
        settle(bias_at(lax.rem(place.core + c, CORES), place.step(place.row, -e)), b_rs.at[i])
    vec[...] = vec_in[0] + vec_in[1]
    for layer in range(2):
        for row in range(side):
            at = pl.ds(row * head, head)
            for t in range(3):
                i = layer * 3 + t
                bq[layer:layer + 1, row * triple + t * head:row * triple + (t + 1) * head] = bias_in[0, i:i + 1, at] + bias_in[1, i:i + 1, at]
            tiles = wide // head
            for t in range(tiles):
                i = 6 + layer * tiles + t
                bu[layer:layer + 1, row * wide + t * head:row * wide + (t + 1) * head] = bias_in[0, i:i + 1, at] + bias_in[1, i:i + 1, at]

    x_ring.forward()
    exchange(1, 0, wq1)
    exchange(1, 1, wu1)
    go.forward()

    tile = min(32, half)

    def norm(src, doc, layer):
        par = [vec[layer * 4 + i:layer * 4 + i + 1, :] for i in range(4)]

        @pl.loop(0, seq, step=tile)
        def _(r):
            at = pl.ds(r, tile)
            rows = src[doc, at, :].astype(f32)
            centered = rows - jnp.mean(rows, axis=-1, keepdims=True)
            var = jnp.mean(centered * centered, axis=-1, keepdims=True)
            normed = centered * lax.rsqrt(var + LN_EPS)
            a_buf[at, :] = (normed * par[0] + par[1]).astype(bf)
            m_buf[doc, at, :] = (normed * par[2] + par[3]).astype(bf)

    def attend(doc, layer):
        chip = place.row * side + doc
        lens = vec[12:13, pl.ds(pl.multiple_of(chip * head, head), head)]
        lane = lax.broadcasted_iota(jnp.int32, (1, head), 1)
        length = jnp.sum(jnp.where(lane == place.core * (head // CORES), lens, 0.0), axis=1, keepdims=True)
        query = lax.broadcasted_iota(jnp.int32, (seq, seq), 0)
        key = lax.broadcasted_iota(jnp.int32, (seq, seq), 1)
        visible = (key <= query) & (key.astype(f32) < length)
        pair = 2 * triple

        def turn(u):
            u = u.astype(f32)
            shift = head // 8
            return (u * rot_ref[0] + pltpu.roll(u, head - shift, 1) * rot_ref[1] + pltpu.roll(u, shift, 1) * rot_ref[2]).astype(bf)

        @pl.loop(0, per // 2)
        def _(p):
            at = pl.ds(pl.multiple_of(p * pair, pair), pair)
            w = wq[:, :, :, :, at].reshape(d_model, pair)
            qkv = (jnp.dot(a_buf[...], w, preferred_element_type=f32) + bq[layer:layer + 1, at]).astype(bf)
            for h in range(2):
                q, k, v = (qkv[:, h * triple + j * head:h * triple + (j + 1) * head] for j in range(3))
                scores = lax.dot_general(turn(q), turn(k), (((1,), (1,)), ((), ())), preferred_element_type=f32) * (head ** -0.5)
                scores = jnp.where(visible, scores, -1e30)
                probs = jnp.exp(scores - jnp.max(scores, axis=-1, keepdims=True))
                probs = (probs / jnp.sum(probs, axis=-1, keepdims=True)).astype(bf)
                to = pl.ds(pl.multiple_of((p * 2 + h) * head, head), head)
                ctx[doc, :, to] = jnp.dot(probs, v, preferred_element_type=f32).astype(bf)

    def up(doc, layer):
        step = ff // 8

        @pl.loop(0, 2)
        def _(n):
            for j in range(4):
                at = pl.ds(pl.multiple_of((n * 4 + j) * step, step), step)
                u = jnp.dot(m_buf[doc], wu[:, :, :, :, at].reshape(d_model, step), preferred_element_type=f32) + bu[layer:layer + 1, at]
                act[doc, :, at] = (0.5 * u * (1.0 + lax.erf(u * (0.5 ** 0.5)))).astype(bf)

    def down(doc, h):
        step = d_cols // 4
        for n in range(4):
            at = pl.ds(n * step, step)
            wide_at = pl.ds(pl.multiple_of(h * d_cols + n * step, step), step)
            tot = jnp.dot(ctx[doc], wo[:, :, :, wide_at].reshape(per * head, step), preferred_element_type=f32)
            part[doc, h, :, at] = tot + jnp.dot(act[doc], wd[h, :, :, :, at].reshape(ff, step), preferred_element_type=f32)

    top, low = pl.ds(0, half), pl.ds(half, half)

    def send_far(layer, h):
        send(part.at[far, h, top], hop_a.at[h], r_ss.at[layer, h, 0], r_rs.at[layer, h, 0], left)
        send(part.at[far, h, low], hop_b.at[h], r_ss.at[layer, h, 1], r_rs.at[layer, h, 1], right)

    def send_prv(layer, h):
        send(part.at[prv, h, low], fin.at[0, h], r_ss.at[layer, h, 2], r_rs.at[layer, h, 2], left)

    def send_nxt(layer, h):
        send(part.at[nxt, h, top], fin.at[1, h], r_ss.at[layer, h, 3], r_rs.at[layer, h, 3], right)

    def pass_on(layer, h):
        for i, hop, doc, first, dev in ((0, hop_a, prv, 0, left), (1, hop_b, nxt, half, right)):
            settle(hop.at[h], r_rs.at[layer, h, i])

            @pl.loop(0, half, step=tile)
            def _(r, hop=hop, doc=doc, first=first):
                hop[h, pl.ds(r, tile), :] = hop[h, pl.ds(r, tile), :] + part[doc, h, pl.ds(first + r, tile), :]

            send(hop.at[h], fin.at[2 + i, h], r_ss.at[layer, h, 4 + i], r_rs.at[layer, h, 4 + i], dev)

    def owner_sums(layer, src, store):
        for h in range(2):
            cols = slice(h * d_cols, (h + 1) * d_cols)
            for i in range(2, 6):
                settle(fin.at[i - 2, h], r_rs.at[layer, h, i])
            for first, f_one, f_two in ((0, 1, 2), (half, 0, 3)):
                @pl.loop(0, half, step=tile)
                def _(r, first=first, f_one=f_one, f_two=f_two):
                    here, at = pl.ds(r, tile), pl.ds(first + r, tile)
                    tot = part[place.col, h, at, :] + fin[f_one, h, here, :] + fin[f_two, h, here, :]
                    bias = vec[8 + layer:9 + layer, cols] + vec[10 + layer:11 + layer, cols]
                    store(at, cols, (src[place.col, at, cols].astype(f32) + (tot + bias)).astype(bf))

    def sums_sent(layer):
        for h in range(2):
            for i in range(6):
                settle(hop_a.at[h], r_ss.at[layer, h, i])

    def nearest_first(i):
        return lax.rem(place.col + jnp.where(i == 0, 0, jnp.where(i == 1, 1, jnp.where(i == 2, side - 1, 2))), side)

    settle(xg.at[place.col], loc.at[0])
    gq.finish()

    @pl.loop(0, side)
    def _(i):
        doc = nearest_first(i)

        @pl.when(i == 1)
        def _():
            x_ring.rest()

        @pl.when(i == 2)
        def _():
            gu.forward()
            gd[0].start()

        @pl.when(i == 3)
        def _():
            x_ring.last()

        norm(xg, doc, 0)
        attend(doc, 0)

    gu.finish()

    @pl.loop(0, side)
    def _(doc):
        up(doc, 0)

        @pl.when(doc == 0)
        def _():
            gd[0].forward()
            gd[1].forward()

        @pl.when(doc == 1)
        def _():
            exchanged(1, 0, wq1)
            exchanged(1, 1, wu1)
            gq1.start()
            gu1.start()

    go.finish()
    settle(wo.at[place.row, place.core], loc.at[1])

    for h in range(2):
        settle(wd.at[h, place.row, place.core], loc.at[3 + h])
        gd[h].finish()

        @pl.loop(0, side)
        def _(i, h=h):
            doc = lax.rem(place.col + jnp.where(i == 0, 2, jnp.where(i == 1, 1, jnp.where(i == 2, side - 1, 0))), side)
            down(doc, h)

            @pl.when(i == 0)
            def _():
                send_far(0, h)

            @pl.when(i == 1)
            def _():
                send_nxt(0, h)

            @pl.when(i == 2)
            def _():
                send_prv(0, h)

    gq1.forward()
    pass_on(0, 0)
    pass_on(0, 1)
    gu1.forward()
    go1.start()
    gd1[0].start()
    gd1[1].start()
    for g in gathers[0]:
        g.drain()
    gq1.finish()
    pltpu.make_async_copy(wq1, wq, loc1.at[0]).start()
    gu1.finish()
    pltpu.make_async_copy(wu1, wu, loc1.at[1]).start()

    def keep(at, cols, rows):
        xg1[place.col, at, cols] = rows

    owner_sums(0, xg, keep)
    x1_ring.start()
    go1.forward()
    sums_sent(0)
    settle(wq, loc1.at[0])
    settle(wu, loc1.at[1])

    @pl.loop(0, side)
    def _(i):
        doc = nearest_first(i)

        @pl.when(i == 1)
        def _():
            x1_ring.rest()

        @pl.when(i == 2)
        def _():
            settle(wo1.at[place.row, place.core], loc.at[2])
            go1.finish()
            pltpu.make_async_copy(wo1, wo, loc1.at[2]).start()
            settle(wd1.at[0, place.row, place.core], loc.at[5])
            gd1[0].finish()
            pltpu.make_async_copy(wd1.at[0], wd.at[0], loc1.at[3]).start()

        @pl.when(i == 3)
        def _():
            x1_ring.last()

        norm(xg1, doc, 1)
        attend(doc, 1)
        up(doc, 1)

        @pl.when(i == 0)
        def _():
            x1_ring.forward()
            gd1[0].forward()
            gd1[1].forward()

        @pl.when(i == 2)
        def _():
            settle(wd1.at[1, place.row, place.core], loc.at[6])
            gd1[1].finish()
            pltpu.make_async_copy(wd1.at[1], wd.at[1], loc1.at[4]).start()
            settle(wo, loc1.at[2])
            settle(wd.at[0], loc1.at[3])
            down(nxt, 0)
            send_nxt(1, 0)
            down(prv, 0)
            send_prv(1, 0)
            settle(wd.at[1], loc1.at[4])
            down(nxt, 1)
            send_nxt(1, 1)
            down(prv, 1)
            send_prv(1, 1)

        @pl.when(i == 3)
        def _():
            for h in range(2):
                down(far, h)
                send_far(1, h)
            for h in range(2):
                down(place.col, h)

    pass_on(1, 0)
    pass_on(1, 1)

    def give_out(at, cols, rows):
        out_ref[at, cols] = rows

    owner_sums(1, xg1, give_out)
    sums_sent(1)
    for g in gathers[1]:
        g.drain()
    x_ring.drain()
    x1_ring.drain()
    for d in range(count - 1):
        settle(vec_ref, v_ss.at[d])
    for i in range(len(column)):
        settle(bias_ref, b_ss.at[i])
    for layer in range(2):
        for kind, buf in enumerate((wq, wu)):
            for d in range(1, side):
                settle(buf.at[0, 0, 0], a_ss.at[layer, kind, d])


VM = pl.BlockSpec(memory_space=pltpu.VMEM)
ANY = pl.BlockSpec(memory_space=pl.ANY)
DMA = pltpu.SemaphoreType.DMA


def solution(mesh):
    row_spec = P(('dp', 'fsdp'), None, None)
    in_specs = (row_spec, P(('dp', 'fsdp')), P(None, None, 'fsdp'), P(None, 'fsdp', None, None), P(None, 'fsdp'), P(None, 'fsdp', None), P(None, 'fsdp'), P(None, 'fsdp', None), P(None, 'fsdp'), P(None, 'fsdp', None), P(None, 'fsdp'))
    count = mesh.shape['fsdp']
    side = math.isqrt(count // CORES)

    def local_step(hidden_loc, lens_loc, ln_par, w_qkv, b_qkv, w_out, b_out, w_up, b_up, w_down, b_down):
        layers = ln_par.shape[0]
        _, seq_len, d_model = hidden_loc.shape
        d_rows, heads, triple = w_qkv.shape[1:]
        head_dim = triple // 3
        per = heads // side
        ff_rows = w_down.shape[1]
        ff = ff_rows * CORES * side
        bf, f32 = jnp.bfloat16, jnp.float32
        core = lax.axis_index('fsdp') % CORES

        def placed(vals):
            zero = jnp.zeros_like(vals)
            return jnp.where(core == 0, jnp.concatenate([vals, zero], axis=-1), jnp.concatenate([zero, vals], axis=-1))

        lens_row = jnp.broadcast_to(lens_loc.astype(f32)[:, None], (1, d_rows))
        vec = jnp.concatenate([ln_par.reshape(-1, d_rows), b_out.astype(f32), b_down.astype(f32), lens_row, jnp.zeros((3, d_rows), f32)], axis=0)
        vec = placed(vec)
        bias = jnp.concatenate([placed(b_qkv.astype(f32)).reshape(-1, head_dim), placed(b_up.astype(f32)).reshape(-1, head_dim)], axis=0)
        bias = jnp.pad(bias, ((0, -bias.shape[0] % 16), (0, 0)))
        wq = w_qkv.reshape(layers, d_rows, per, side, triple).transpose(0, 3, 1, 2, 4).reshape(layers, side, d_rows, per * triple)

        half = seq_len // 2
        wq_s, wu_s = (side, side, CORES, d_rows, per * triple), (side, side, CORES, d_rows, ff)
        wo_s, wd_s = (side, CORES) + w_out.shape[1:], (2, side, CORES, ff_rows, d_model // 2)
        outs = pl.pallas_call(
            functools.partial(both_layers, side),
            out_shape=(jax.ShapeDtypeStruct((seq_len, d_model), bf), *(jax.ShapeDtypeStruct(s, bf) for s in (wq_s, wu_s, wo_s, wd_s))),
            in_specs=[ANY, VM, VM, VM, ANY, ANY, ANY, ANY],
            out_specs=(VM, ANY, ANY, ANY, ANY),
            scratch_shapes=[
                *(pltpu.VMEM(s, bf) for s in (wq_s, wu_s, wo_s, wd_s)),
                pltpu.VMEM((side, seq_len, d_model), bf),
                pltpu.VMEM((side, seq_len, d_model), bf),
                pltpu.VMEM((seq_len, d_model), bf),
                pltpu.VMEM((side, seq_len, d_model), bf),
                pltpu.VMEM((side, seq_len, ff), bf),
                pltpu.VMEM((side, seq_len, per * head_dim), bf),
                pltpu.VMEM((side, 2, seq_len, d_model // 2), f32),
                pltpu.VMEM((2, half, d_model // 2), f32),
                pltpu.VMEM((2, half, d_model // 2), f32),
                pltpu.VMEM((4, 2, half, d_model // 2), f32),
                pltpu.VMEM((CORES, 16, d_model), f32),
                pltpu.VMEM((CORES, bias.shape[0], side * head_dim), f32),
                pltpu.VMEM((16, d_model), f32),
                pltpu.VMEM((layers, per * triple), f32),
                pltpu.VMEM((layers, ff), f32),
                DMA((count - 1,)), DMA((count - 1,)), DMA((side * CORES - 1,)), DMA((side * CORES - 1,)),
                DMA((2, 6)), DMA((2, 6)), DMA((2, 2, side)), DMA((2, 2, side)),
                DMA((2, 5, 6)), DMA((2, 5, 6)), DMA((2, 5, 8)), DMA((2, 5, 8)),
                DMA((2, 2, 6)), DMA((2, 2, 6)), DMA((7,)), DMA((5,)),
            ],
            compiler_params=pltpu.CompilerParams(collective_id=0, has_side_effects=True, vmem_limit_bytes=67043328),
        )(hidden_loc[0], vec, bias, rotary_factors(seq_len, head_dim), wq, w_up, w_out, w_down)
        return outs[0][None]

    return jax.shard_map(local_step, mesh=mesh, in_specs=in_specs, out_specs=row_spec, check_vma=False)
```

```python
import functools
import math

import jax
import jax.numpy as jnp
import numpy as np
from jax import lax
from jax.experimental import pallas as pl
from jax.experimental.pallas import tpu as pltpu
from jax.sharding import PartitionSpec as P

ROPE_BASE = 10000.0
LN_EPS = 1e-5
CORES = 2
MESH = pl.DeviceIdType.MESH


def rotary_factors(seq_len, head_dim):
    rot = head_dim // 4
    half = rot // 2
    inv_freq = (1.0 / (ROPE_BASE ** (np.arange(0, rot, 2, dtype=np.float32) / rot))).astype(np.float32)
    angles = np.arange(seq_len, dtype=np.float32)[:, None] * inv_freq[None, :]
    cos, sin = np.cos(angles), np.sin(angles)
    out = np.zeros((3, seq_len, head_dim), np.float32)
    out[0] = 1.0
    out[0, :, :half], out[0, :, half:rot] = cos, cos
    out[1, :, :half] = -sin
    out[2, :, half:rot] = sin
    return jnp.asarray(out)


def send(src, dst, send_sem, recv_sem, dev):
    pltpu.make_async_remote_copy(src_ref=src, dst_ref=dst, send_sem=send_sem, recv_sem=recv_sem, device_id={"fsdp": dev}, device_id_type=MESH).start()


def settle(ref, sem):
    pltpu.make_async_copy(ref, ref, sem).wait()


class Place:
    def __init__(self, side):
        me = lax.axis_index("fsdp")
        self.side, self.me = side, me
        self.core = lax.rem(me, CORES)
        self.chip = me // CORES
        self.col = lax.rem(self.chip, side)
        self.row = self.chip // side
        self.sib = self.dev(self.row, self.col, 1 - self.core)

    def dev(self, row, col, core):
        return (row * self.side + col) * CORES + core

    def step(self, pos, by):
        return lax.rem(pos + by + self.side, self.side)

    def in_row(self, by):
        return self.dev(self.row, self.step(self.col, by), self.core)

    def in_col(self, by):
        return self.dev(self.step(self.row, by), self.col, self.core)


class Ring:
    def __init__(self, place, pos, right, left, blk, own, ss, rs):
        self.pos, self.right, self.left, self.blk, self.own, self.ss, self.rs = pos, right, left, blk, own, ss, rs
        self.prev, self.next, self.far = place.step(pos, -1), place.step(pos, 1), place.step(pos, 2)

    def _send(self, src, pos, half, i, j, dev):
        send(src, self.blk(pos, half), self.ss.at[i], self.rs.at[j], dev)

    def start(self):
        self._send(self.own(0), self.pos, 0, 0, 0, self.right)
        self._send(self.own(1), self.pos, 1, 2, 3, self.left)
        self._send(self.own(1), self.pos, 1, 1, 1, self.right)
        self._send(self.own(0), self.pos, 0, 3, 2, self.left)

    def forward(self):
        settle(self.blk(self.prev, 0), self.rs.at[0])
        self._send(self.blk(self.prev, 0), self.prev, 0, 4, 4, self.right)
        settle(self.blk(self.next, 1), self.rs.at[3])
        self._send(self.blk(self.next, 1), self.next, 1, 5, 5, self.left)

    def rest(self):
        settle(self.blk(self.prev, 1), self.rs.at[1])
        settle(self.blk(self.next, 0), self.rs.at[2])

    def last(self):
        settle(self.blk(self.far, 0), self.rs.at[4])
        settle(self.blk(self.far, 1), self.rs.at[5])

    def drain(self):
        for i, half in enumerate((0, 1, 1, 0, 0, 1)):
            settle(self.blk(self.pos, half), self.ss.at[i])


class Gather:
    def __init__(self, place, blk, own, ss, rs, cs, cr):
        mine = lambda row, half: blk(row, half, place.core)
        self.theirs = lambda row, half: blk(row, half, 1 - place.core)
        own = own if own is not None else (lambda half: mine(place.row, half))
        self.ring = Ring(place, place.row, place.in_col(1), place.in_col(-1), mine, own, ss, rs)
        self.sib, self.cs, self.cr = place.sib, cs, cr
        self.blocks = (self.ring.pos, self.ring.prev, self.ring.next, self.ring.far)

    def give(self, rel, half, src=None):
        i = rel * 2 + half
        blk = self.ring.blk(self.blocks[rel], half)
        send(blk if src is None else src, blk, self.cs.at[i], self.cr.at[i], self.sib)

    def start(self):
        self.ring.start()

    def own(self):
        self.give(0, 0, self.ring.own(0))
        self.give(0, 1, self.ring.own(1))

    def forward(self):
        self.ring.forward()
        self.give(1, 0)
        self.give(2, 1)

    def hand(self):
        self.ring.rest()
        self.give(1, 1)
        self.give(2, 0)

    def tail(self):
        self.ring.last()
        self.give(3, 0)
        self.give(3, 1)

    def take(self):
        for rel in range(4):
            for half in range(2):
                settle(self.theirs(self.blocks[rel], half), self.cr.at[rel * 2 + half])

    def drain(self):
        self.ring.drain()
        for rel in range(4):
            for half in range(2):
                settle(self.ring.blk(self.blocks[rel], half), self.cs.at[rel * 2 + half])


def weight_gathers(place, bufs, wo_own, wd_own, sems):
    wq, wu, wo, wd = bufs
    cols = wq.shape[1] // 2
    o_rows, d_rows, d_cols = wo.shape[2] // 2, wd.shape[3] // 2, wd.shape[4]
    specs = (
        (lambda row, half, core: wq.at[row, pl.ds(half * cols, cols), core], None),
        (lambda row, half, core: wu.at[row, pl.ds(half * cols, cols), core], None),
        (lambda row, half, core: wo.at[row, core, pl.ds(half * o_rows, o_rows)], lambda half: wo_own.at[pl.ds(half * o_rows, o_rows)]),
        *((lambda row, half, core, h=h: wd.at[h, row, core, pl.ds(half * d_rows, d_rows)],
           lambda half, h=h: wd_own.at[pl.ds(half * d_rows, d_rows), pl.ds(h * d_cols, d_cols)]) for h in range(2)),
    )
    return [Gather(place, blk, own, *(s.at[t] for s in sems)) for t, (blk, own) in enumerate(specs)]


def both_layers(side, x_ref, lens_ref, ln_ref, bq_ref, bo_ref, bu_ref, bd_ref, rot_ref, wq_ref, wu_ref, wo_ref, wd_ref,
                out_ref, wq1, wu1, wo1, wd1,
                wq, wu, wo, wd, xg, xg1, a_buf, m_buf, act, ctx, part, hop_a, hop_b, fin, vec_own, bias_own, bq_pad, vec_in, bias_in, vec, bq, bu,
                v_ss, v_rs, b_ss, b_rs, x_ss, x_rs, a_ss, a_rs, w_ss, w_rs, c_ss, c_rs, r_ss, r_rs, loc, loc1):
    f32, bf = jnp.float32, jnp.bfloat16
    place = Place(side)
    count = side * side * CORES
    seq, d_model = x_ref.shape
    head = rot_ref.shape[2]
    triple = 3 * head
    per = side
    ff = act.shape[2]
    half = seq // 2
    wide = wu_ref.shape[2] // (side * side)
    right, left = place.in_row(1), place.in_row(-1)
    nxt, prv, far = place.step(place.col, 1), place.step(place.col, -1), place.step(place.col, 2)

    second = place.core == 1
    width = head // CORES
    vec_own[...] = jnp.zeros_like(vec_own)
    for layer in range(2):
        vec_own[layer * 4:layer * 4 + 4, :width] = ln_ref[layer]
    vec_own[8:10, :width] = bo_ref[...].astype(f32)
    vec_own[10:12, :width] = bd_ref[...].astype(f32)
    vec_own[12:13, :width] = jnp.full((1, width), lens_ref[0].astype(f32))
    rows = vec_own[...]
    vec_own[...] = jnp.where(second, pltpu.roll(rows, width, 1), rows)
    bq_pad[...] = jnp.zeros_like(bq_pad)
    bq_pad[:, :3 * width] = bq_ref[...].astype(f32)
    lead, rest = bq_pad[:, :head], bq_pad[:, head:]
    lead_turned, rest_turned = pltpu.roll(lead, width, 1), pltpu.roll(rest, width, 1)
    upper = lax.broadcasted_iota(jnp.int32, lead.shape, 1) >= width
    q_tiles = (jnp.where(second, 0.0, lead), jnp.where(second, jnp.where(upper, lead_turned, 0.0), rest),
               jnp.where(second, jnp.where(upper, rest_turned, lead_turned), 0.0))
    tiles = wide // head
    bias_own[...] = jnp.zeros_like(bias_own)
    for layer in range(2):
        for t in range(3):
            bias_own[layer * 3 + t:layer * 3 + t + 1, :] = q_tiles[t][layer:layer + 1]
        for t in range(tiles):
            t_core, t_at = t // (tiles // CORES), t % (tiles // CORES)
            part_of = bu_ref[layer:layer + 1, t_at * head:(t_at + 1) * head].astype(f32)
            bias_own[6 + layer * tiles + t:7 + layer * tiles + t, :] = jnp.where(place.core == t_core, part_of, 0.0)

    barrier = pltpu.get_barrier_semaphore()
    others = [lax.rem(place.me + d, count) for d in range(1, count)]
    for dev in others:
        pl.semaphore_signal(barrier, inc=1, device_id={"fsdp": dev}, device_id_type=MESH)
    pl.semaphore_wait(barrier, count - 1)

    def exchange(layer, kind, dst_buf):
        for d in (1, 3, 2, 0):
            col = place.step(place.col, d)
            dst = dst_buf.at[place.row, place.col, place.core]
            src_ref, size = (wu_ref, wide) if kind else (wq_ref, triple)
            for k in range(side):
                off = pl.multiple_of((k * side + col) * size, size)
                src, to = src_ref.at[layer, :, pl.ds(off, size)], dst.at[:, pl.ds(k * size, size)]
                if d:
                    send(src, to, a_ss.at[layer, kind, d], a_rs.at[layer, kind, d], place.in_row(d))
                else:
                    pltpu.make_async_copy(src, to, a_rs.at[layer, kind, d]).start()

    def exchanged(layer, kind, dst_buf):
        for d in range(side):
            settle(dst_buf.at[place.row, place.step(place.col, -d), place.core], a_rs.at[layer, kind, d])

    gathers = [
        weight_gathers(place, (wq, wu, wo, wd), wo_ref.at[0], wd_ref.at[0], [s.at[0] for s in (w_ss, w_rs, c_ss, c_rs)]),
        weight_gathers(place, (wq1, wu1, wo1, wd1), wo_ref.at[1], wd_ref.at[1], [s.at[1] for s in (w_ss, w_rs, c_ss, c_rs)]),
    ]
    gq, gu, go, *gd = gathers[0]
    gq1, gu1, go1, *gd1 = gathers[1]
    d_cols = wd.shape[4]
    rows_of = lambda ref, col, h: ref.at[col, pl.ds(h * half, half)]
    x_ring = Ring(place, place.col, right, left, lambda col, h: rows_of(xg, col, h), lambda h: x_ref.at[pl.ds(h * half, half)], x_ss.at[0, 0], x_rs.at[0, 0])
    x1_at = lambda h: lambda col, half_at: xg1.at[col, pl.ds(half_at * half, half), pl.ds(h * d_cols, d_cols)]
    x1_rings = [Ring(place, place.col, right, left, x1_at(h), lambda half_at, h=h: x1_at(h)(place.col, half_at), x_ss.at[1, h], x_rs.at[1, h]) for h in range(2)]

    exchange(0, 0, wq)
    vec_at = lambda core, chip: vec_in.at[core, :, pl.ds(pl.multiple_of(chip * head, head), head)]
    bias_at = lambda core, row: bias_in.at[core, :, pl.ds(pl.multiple_of(row * head, head), head)]
    for d, dev in enumerate(others):
        send(vec_own, vec_at(place.core, place.chip), v_ss.at[d], v_rs.at[d], dev)
    column = [(e, c) for e in range(side) for c in range(CORES) if e or c]
    for i, (e, c) in enumerate(column):
        dev = place.dev(place.step(place.row, e), place.col, lax.rem(place.core + c, CORES))
        send(bias_own, bias_at(place.core, place.row), b_ss.at[i], b_rs.at[i], dev)
    exchange(0, 1, wu)
    for g in (go, gd[1]):
        g.start()
        g.own()
    x_ring.start()
    own = [(x_ref, xg.at[place.col]), (wo_ref.at[0], wo.at[place.row, place.core]), (wo_ref.at[1], wo1.at[place.row, place.core])]
    own += [(wd_ref.at[layer, :, pl.ds(h * d_cols, d_cols)], buf.at[h, place.row, place.core]) for layer, buf in enumerate((wd, wd1)) for h in range(2)]
    for i, (src, dst) in enumerate(own):
        pltpu.make_async_copy(src, dst, loc.at[i]).start()

    vec_in[place.core, :, pl.ds(pl.multiple_of(place.chip * head, head), head)] = vec_own[...]
    bias_in[place.core, :, pl.ds(pl.multiple_of(place.row * head, head), head)] = bias_own[...]

    exchanged(0, 0, wq)
    gq.start()
    gq.own()
    exchanged(0, 1, wu)
    gq.forward()
    gu.start()
    gu.own()

    for d in range(1, count):
        src = lax.rem(place.me + count - d, count)
        settle(vec_at(lax.rem(src, CORES), src // CORES), v_rs.at[d - 1])
    for i, (e, c) in enumerate(column):
        settle(bias_at(lax.rem(place.core + c, CORES), place.step(place.row, -e)), b_rs.at[i])
    vec[...] = vec_in[0] + vec_in[1]
    for layer in range(2):
        for row in range(side):
            at = pl.ds(row * head, head)
            rows = bias_in[0, :, at] + bias_in[1, :, at]
            for tall, out, first, n in ((triple, bq, 0, 3), (wide, bu, 6, tiles)):
                for t in range(n):
                    i = first + layer * n + t
                    out[layer:layer + 1, row * tall + t * head:row * tall + (t + 1) * head] = rows[i:i + 1]

    x_ring.forward()
    exchange(1, 0, wq1)
    exchange(1, 1, wu1)
    go.forward()
    gq.hand()

    tile = min(32, half)

    def norm(src, doc, layer, to, halves=(0, 1)):
        par = [vec[layer * 4 + i:layer * 4 + i + 1, :] for i in range(4)]

        @pl.loop(halves[0] * half, (halves[-1] + 1) * half, step=tile)
        def _(r):
            at = pl.ds(r, tile)
            rows = src[doc, at, :].astype(f32)
            centered = rows - jnp.mean(rows, axis=-1, keepdims=True)
            var = jnp.mean(centered * centered, axis=-1, keepdims=True)
            normed = centered * lax.rsqrt(var + LN_EPS)
            to[at, :] = (normed * par[0] + par[1]).astype(bf)
            m_buf[doc, at, :] = (normed * par[2] + par[3]).astype(bf)

    def attend(doc, layer, rows):
        chip = place.row * side + doc
        lens = vec[12:13, pl.ds(pl.multiple_of(chip * head, head), head)]
        lane = lax.broadcasted_iota(jnp.int32, (1, head), 1)
        length = jnp.sum(jnp.where(lane == place.core * (head // CORES), lens, 0.0), axis=1, keepdims=True)
        query = lax.broadcasted_iota(jnp.int32, (seq, seq), 0)
        key = lax.broadcasted_iota(jnp.int32, (seq, seq), 1)
        visible = (key <= query) & (key.astype(f32) < length)
        pair = 2 * triple

        def turn(u):
            u = u.astype(f32)
            shift = head // 8
            return (u * rot_ref[0] + pltpu.roll(u, head - shift, 1) * rot_ref[1] + pltpu.roll(u, shift, 1) * rot_ref[2]).astype(bf)

        @pl.loop(0, per // 2)
        def _(p):
            at = pl.ds(pl.multiple_of(p * pair, pair), pair)
            w = wq[:, :, :, :, at].reshape(d_model, pair)
            qkv = (jnp.dot(rows[...], w, preferred_element_type=f32) + bq[layer:layer + 1, at]).astype(bf)
            for h in range(2):
                q, k, v = (qkv[:, h * triple + j * head:h * triple + (j + 1) * head] for j in range(3))
                scores = lax.dot_general(turn(q), turn(k), (((1,), (1,)), ((), ())), preferred_element_type=f32) * (head ** -0.5)
                scores = jnp.where(visible, scores, -1e30)
                probs = jnp.exp(scores - jnp.max(scores, axis=-1, keepdims=True))
                probs = (probs / jnp.sum(probs, axis=-1, keepdims=True)).astype(bf)
                to = pl.ds(pl.multiple_of((p * 2 + h) * head, head), head)
                ctx[doc, :, to] = jnp.dot(probs, v, preferred_element_type=f32).astype(bf)

    def up(doc, layer):
        step = ff // 8

        @pl.loop(0, 2)
        def _(n):
            for j in range(4):
                at = pl.ds(pl.multiple_of((n * 4 + j) * step, step), step)
                u = jnp.dot(m_buf[doc], wu[:, :, :, :, at].reshape(d_model, step), preferred_element_type=f32) + bu[layer:layer + 1, at]
                act[doc, :, at] = (0.5 * u * (1.0 + lax.erf(u * (0.5 ** 0.5)))).astype(bf)

    def down(doc, h):
        step = d_cols // 4
        for n in range(4):
            at = pl.ds(n * step, step)
            wide_at = pl.ds(pl.multiple_of(h * d_cols + n * step, step), step)
            tot = jnp.dot(ctx[doc], wo[:, :, :, wide_at].reshape(per * head, step), preferred_element_type=f32)
            part[doc, h, :, at] = tot + jnp.dot(act[doc], wd[h, :, :, :, at].reshape(ff, step), preferred_element_type=f32)

    top, low = pl.ds(0, half), pl.ds(half, half)

    def send_part(layer, h, i, doc, rows, to, dev):
        send(part.at[doc, h, rows], to.at[h], r_ss.at[layer, h, i], r_rs.at[layer, h, i], dev)

    def send_far(layer, h):
        send_part(layer, h, 0, far, top, hop_a, left)
        send_part(layer, h, 1, far, low, hop_b, right)

    def send_prv(layer, h):
        send_part(layer, h, 2, prv, low, fin.at[0], left)

    def send_nxt(layer, h):
        send_part(layer, h, 3, nxt, top, fin.at[1], right)

    def pass_on(layer, h):
        for i, hop, doc, first, dev in ((0, hop_a, prv, 0, left), (1, hop_b, nxt, half, right)):
            settle(hop.at[h], r_rs.at[layer, h, i])

            @pl.loop(0, half, step=tile)
            def _(r, hop=hop, doc=doc, first=first):
                hop[h, pl.ds(r, tile), :] = hop[h, pl.ds(r, tile), :] + part[doc, h, pl.ds(first + r, tile), :]

            send(hop.at[h], fin.at[2 + i, h], r_ss.at[layer, h, 4 + i], r_rs.at[layer, h, 4 + i], dev)

    def owner_sums(layer, src, store, done):
        for h in range(2):
            cols = slice(h * d_cols, (h + 1) * d_cols)
            for i in range(2, 6):
                settle(fin.at[i - 2, h], r_rs.at[layer, h, i])
            for first, f_one, f_two in ((0, 1, 2), (half, 0, 3)):
                @pl.loop(0, half, step=tile)
                def _(r, first=first, f_one=f_one, f_two=f_two):
                    here, at = pl.ds(r, tile), pl.ds(first + r, tile)
                    tot = part[place.col, h, at, :] + fin[f_one, h, here, :] + fin[f_two, h, here, :]
                    bias = vec[8 + layer:9 + layer, cols] + vec[10 + layer:11 + layer, cols]
                    store(at, cols, (src[place.col, at, cols].astype(f32) + (tot + bias)).astype(bf))

            done(h)

    def sums_sent(layer):
        for h in range(2):
            for i in range(6):
                settle(hop_a.at[h], r_ss.at[layer, h, i])

    def chosen(i, docs):
        doc = docs[-1]
        for at, other in enumerate(docs[:-1]):
            doc = jnp.where(i == at, other, doc)
        return doc

    mine = place.col
    nearest_first = (mine, nxt, prv, far)
    farthest_first = (far, nxt, prv, mine)

    settle(xg.at[place.col], loc.at[0])
    gq.tail()
    gq.take()

    @pl.loop(0, side)
    def _(i):
        doc = chosen(i, nearest_first)

        @pl.when(i == 1)
        def _():
            x_ring.rest()

        @pl.when(i == 2)
        def _():
            gu.forward()
            gd[0].start()
            gd[0].own()
            go.hand()

        @pl.when(i == 3)
        def _():
            x_ring.last()
            gu.hand()

        norm(xg, doc, 0, a_buf)
        attend(doc, 0, a_buf)

    gd[1].hand()
    go.tail()
    gu.tail()
    gu.take()

    @pl.loop(0, side)
    def _(doc):
        up(doc, 0)

        @pl.when(doc == 0)
        def _():
            gd[0].forward()
            gd[1].forward()

        @pl.when(doc == 2)
        def _():
            gd[0].hand()

    gd[0].tail()
    exchanged(1, 0, wq1)
    exchanged(1, 1, wu1)
    gq1.start()
    gu1.start()
    settle(wo.at[place.row, place.core], loc.at[1])
    go.take()

    for h in range(2):
        settle(wd.at[h, place.row, place.core], loc.at[3 + h])
        gd[h].take()

        @pl.loop(0, side)
        def _(i, h=h):
            doc = chosen(i, farthest_first)
            down(doc, h)

            @pl.when(i == 0)
            def _():
                send_far(0, h)

            @pl.when(i == 1)
            def _():
                send_nxt(0, h)
                if h == 0:
                    gd[1].tail()

            @pl.when(i == 2)
            def _():
                send_prv(0, h)

    gq1.own()
    gu1.own()
    gq1.forward()
    pass_on(0, 0)
    gu1.forward()
    for g in (go1, *gd1):
        g.start()
        g.own()
    pass_on(0, 1)
    for g in gathers[0]:
        g.drain()
    gq1.hand()
    gq1.tail()
    gu1.hand()
    gq1.take()
    pltpu.make_async_copy(wq1, wq, loc1.at[0]).start()
    gu1.tail()
    gu1.take()
    pltpu.make_async_copy(wu1, wu, loc1.at[1]).start()

    def keep(at, cols, rows):
        xg1[place.col, at, cols] = rows

    owner_sums(0, xg, keep, lambda h: x1_rings[h].start())
    go1.forward()
    gd1[0].forward()
    sums_sent(0)
    x_ring.drain()
    settle(wq, loc1.at[0])
    settle(wu, loc1.at[1])

    norm(xg1, place.col, 1, xg.at[place.col])

    @pl.loop(0, side)
    def _(i):
        doc = chosen(i, nearest_first)

        @pl.when(i == 1)
        def _():
            for ring in x1_rings:
                ring.rest()
            norm(xg1, nxt, 1, xg.at[nxt], (0,))

        @pl.when(i == 3)
        def _():
            for ring in x1_rings:
                ring.last()
            norm(xg1, far, 1, xg.at[far])

        attend(doc, 1, xg.at[doc])

        @pl.when(i == 1)
        def _():
            gd1[0].tail()
            gd1[1].hand()

        @pl.when(i == 2)
        def _():
            gd1[1].tail()

        up(doc, 1)

        @pl.when(i == 0)
        def _():
            for ring in x1_rings:
                ring.forward()
            gd1[1].forward()
            norm(xg1, nxt, 1, xg.at[nxt], (1,))
            norm(xg1, prv, 1, xg.at[prv], (0,))
            go1.hand()
            gd1[0].hand()
            go1.tail()
            settle(wo1.at[place.row, place.core], loc.at[2])
            go1.take()
            pltpu.make_async_copy(wo1, wo, loc1.at[2]).start()

        @pl.when(i == 1)
        def _():
            settle(wd1.at[0, place.row, place.core], loc.at[5])
            gd1[0].take()
            pltpu.make_async_copy(wd1.at[0], wd.at[0], loc1.at[3]).start()
            norm(xg1, prv, 1, xg.at[prv], (1,))
            settle(wo, loc1.at[2])
            settle(wd.at[0], loc1.at[3])
            down(nxt, 0)
            send_nxt(1, 0)

        @pl.when(i == 2)
        def _():
            settle(wd1.at[1, place.row, place.core], loc.at[6])
            gd1[1].take()
            pltpu.make_async_copy(wd1.at[1], wd.at[1], loc1.at[4]).start()
            down(prv, 0)
            send_prv(1, 0)
            settle(wd.at[1], loc1.at[4])
            down(nxt, 1)
            send_nxt(1, 1)
            down(prv, 1)
            send_prv(1, 1)

        @pl.when(i == 3)
        def _():
            for h in range(2):
                down(far, h)
                send_far(1, h)
            for h in range(2):
                down(place.col, h)

    pass_on(1, 0)
    pass_on(1, 1)

    def give_out(at, cols, rows):
        out_ref[at, cols] = rows

    owner_sums(1, xg1, give_out, lambda h: None)
    sums_sent(1)
    for g in gathers[1]:
        g.drain()
    for ring in x1_rings:
        ring.drain()
    for d in range(count - 1):
        settle(vec_own, v_ss.at[d])
    for i in range(len(column)):
        settle(bias_own, b_ss.at[i])
    for layer in range(2):
        for kind, buf in enumerate((wq, wu)):
            for d in range(1, side):
                settle(buf.at[0, 0, 0], a_ss.at[layer, kind, d])


VM = pl.BlockSpec(memory_space=pltpu.VMEM)
ANY = pl.BlockSpec(memory_space=pl.ANY)
DMA = pltpu.SemaphoreType.DMA


def solution(mesh):
    row_spec = P(('dp', 'fsdp'))
    inner = P(None, 'fsdp')
    in_specs = (row_spec, P(('dp', 'fsdp')), P(None, *inner)) + (inner,) * len(('w_qkv', 'b_qkv', 'w_out', 'b_out', 'w_up', 'b_up', 'w_down', 'b_down'))
    count = mesh.shape['fsdp']
    side = math.isqrt(count // CORES)

    def local_step(hidden_loc, lens_loc, ln_par, w_qkv, b_qkv, w_out, b_out, w_up, b_up, w_down, b_down):
        layers = ln_par.shape[0]
        _, seq_len, d_model = hidden_loc.shape
        d_rows, heads, triple = w_qkv.shape[1:]
        head_dim = triple // 3
        per = heads // side
        ff_rows = w_down.shape[1]
        ff = ff_rows * CORES * side
        bf, f32 = jnp.bfloat16, jnp.float32
        wq = w_qkv.reshape(layers, d_rows, heads * triple)
        bias_rows = -(-layers * (3 + ff // side // head_dim) // 16) * 16

        half = seq_len // 2
        wq_s, wu_s = (side, side, CORES, d_rows, per * triple), (side, side, CORES, d_rows, ff)
        wo_s, wd_s = (side, CORES) + w_out.shape[1:], (2, side, CORES, ff_rows, d_model // 2)
        outs = pl.pallas_call(
            functools.partial(both_layers, side),
            out_shape=(jax.ShapeDtypeStruct((seq_len, d_model), bf), *(jax.ShapeDtypeStruct(s, bf) for s in (wq_s, wu_s, wo_s, wd_s))),
            in_specs=[ANY, pl.BlockSpec(memory_space=pltpu.SMEM), VM, VM, VM, VM, VM, VM, ANY, ANY, ANY, ANY],
            out_specs=(VM, ANY, ANY, ANY, ANY),
            scratch_shapes=[
                *(pltpu.VMEM(s, bf) for s in (wq_s, wu_s, wo_s, wd_s)),
                pltpu.VMEM((side, seq_len, d_model), bf),
                pltpu.VMEM((side, seq_len, d_model), bf),
                pltpu.VMEM((seq_len, d_model), bf),
                pltpu.VMEM((side, seq_len, d_model), bf),
                pltpu.VMEM((side, seq_len, ff), bf),
                pltpu.VMEM((side, seq_len, per * head_dim), bf),
                pltpu.VMEM((side, 2, seq_len, d_model // 2), f32),
                pltpu.VMEM((2, half, d_model // 2), f32),
                pltpu.VMEM((2, half, d_model // 2), f32),
                pltpu.VMEM((4, 2, half, d_model // 2), f32),
                pltpu.VMEM((16, head_dim), f32),
                pltpu.VMEM((bias_rows, head_dim), f32),
                pltpu.VMEM((layers, 2 * head_dim), f32),
                pltpu.VMEM((CORES, 16, d_model), f32),
                pltpu.VMEM((CORES, bias_rows, side * head_dim), f32),
                pltpu.VMEM((16, d_model), f32),
                pltpu.VMEM((layers, per * triple), f32),
                pltpu.VMEM((layers, ff), f32),
                *([DMA((count - 1,))] * 2), *([DMA((side * CORES - 1,))] * 2),
                *([DMA((layers, 2, 6))] * 2), *([DMA((layers, 2, side))] * 2),
                *([DMA((layers, 5, 6))] * 2), *([DMA((layers, 5, 8))] * 2),
                *([DMA((layers, 2, 6))] * 2), DMA((7,)), DMA((5,)),
            ],
            compiler_params=pltpu.CompilerParams(collective_id=0, has_side_effects=True, vmem_limit_bytes=67043328),
        )(hidden_loc[0], lens_loc, ln_par, b_qkv, b_out, b_up, b_down, rotary_factors(seq_len, head_dim), wq, w_up, w_out, w_down)
        return outs[0][None]

    return jax.shard_map(local_step, mesh=mesh, in_specs=in_specs, out_specs=row_spec, check_vma=False)
```

```python
import functools
import math

import jax
import jax.numpy as jnp
import numpy as np
from jax import lax
from jax.experimental import pallas as pl
from jax.experimental.pallas import tpu as pltpu
from jax.sharding import PartitionSpec as P

ROPE_BASE = 10000.0
LN_EPS = 1e-5
CORES = 2
MESH = pl.DeviceIdType.MESH


def rotary_factors(seq_len, head_dim):
    rot = head_dim // 4
    half = rot // 2
    inv_freq = (1.0 / (ROPE_BASE ** (np.arange(0, rot, 2, dtype=np.float32) / rot))).astype(np.float32)
    angles = np.arange(seq_len, dtype=np.float32)[:, None] * inv_freq[None, :]
    cos, sin = np.cos(angles), np.sin(angles)
    out = np.zeros((3, seq_len, head_dim), np.float32)
    out[0] = 1.0
    out[0, :, :half], out[0, :, half:rot] = cos, cos
    out[1, :, :half] = -sin
    out[2, :, half:rot] = sin
    return jnp.asarray(out)


def send(src, dst, send_sem, recv_sem, dev):
    pltpu.make_async_remote_copy(src_ref=src, dst_ref=dst, send_sem=send_sem, recv_sem=recv_sem, device_id={"fsdp": dev}, device_id_type=MESH).start()


def settle(ref, sem):
    pltpu.make_async_copy(ref, ref, sem).wait()


class Place:
    def __init__(self, side):
        me = lax.axis_index("fsdp")
        self.side, self.me = side, me
        self.core = lax.rem(me, CORES)
        self.chip = me // CORES
        self.col = lax.rem(self.chip, side)
        self.row = self.chip // side
        self.sib = self.dev(self.row, self.col, 1 - self.core)

    def dev(self, row, col, core):
        return (row * self.side + col) * CORES + core

    def step(self, pos, by):
        return lax.rem(pos + by + self.side, self.side)

    def in_row(self, by):
        return self.dev(self.row, self.step(self.col, by), self.core)

    def in_col(self, by):
        return self.dev(self.step(self.row, by), self.col, self.core)


class Ring:
    def __init__(self, place, pos, right, left, blk, own, ss, rs):
        self.pos, self.right, self.left, self.blk, self.own, self.ss, self.rs = pos, right, left, blk, own, ss, rs
        self.prev, self.next, self.far = place.step(pos, -1), place.step(pos, 1), place.step(pos, 2)

    def _send(self, src, pos, half, i, j, dev):
        send(src, self.blk(pos, half), self.ss.at[i], self.rs.at[j], dev)

    def start(self):
        self._send(self.own(0), self.pos, 0, 0, 0, self.right)
        self._send(self.own(1), self.pos, 1, 2, 3, self.left)
        self._send(self.own(1), self.pos, 1, 1, 1, self.right)
        self._send(self.own(0), self.pos, 0, 3, 2, self.left)

    def forward(self):
        settle(self.blk(self.prev, 0), self.rs.at[0])
        self._send(self.blk(self.prev, 0), self.prev, 0, 4, 4, self.right)
        settle(self.blk(self.next, 1), self.rs.at[3])
        self._send(self.blk(self.next, 1), self.next, 1, 5, 5, self.left)

    def rest(self):
        settle(self.blk(self.prev, 1), self.rs.at[1])
        settle(self.blk(self.next, 0), self.rs.at[2])

    def last(self):
        settle(self.blk(self.far, 0), self.rs.at[4])
        settle(self.blk(self.far, 1), self.rs.at[5])

    def drain(self):
        for i, half in enumerate((0, 1, 1, 0, 0, 1)):
            settle(self.blk(self.pos, half), self.ss.at[i])


class Gather:
    def __init__(self, place, blk, own, ss, rs, cs, cr):
        mine = lambda row, half: blk(row, half, place.core)
        self.theirs = lambda row, half: blk(row, half, 1 - place.core)
        own = own if own is not None else (lambda half: mine(place.row, half))
        self.ring = Ring(place, place.row, place.in_col(1), place.in_col(-1), mine, own, ss, rs)
        self.sib, self.cs, self.cr = place.sib, cs, cr
        self.blocks = (self.ring.pos, self.ring.prev, self.ring.next, self.ring.far)

    def give(self, rel, half, src=None):
        i = rel * 2 + half
        blk = self.ring.blk(self.blocks[rel], half)
        send(blk if src is None else src, blk, self.cs.at[i], self.cr.at[i], self.sib)

    def start(self):
        self.ring.start()

    def own(self):
        self.give(0, 0, self.ring.own(0))
        self.give(0, 1, self.ring.own(1))

    def forward(self):
        self.ring.forward()
        self.give(1, 0)
        self.give(2, 1)

    def hand(self):
        self.ring.rest()
        self.give(1, 1)
        self.give(2, 0)

    def tail(self):
        self.ring.last()
        self.give(3, 0)
        self.give(3, 1)

    def take(self):
        for rel in range(4):
            for half in range(2):
                settle(self.theirs(self.blocks[rel], half), self.cr.at[rel * 2 + half])

    def drain(self):
        self.ring.drain()
        for rel in range(4):
            for half in range(2):
                settle(self.ring.blk(self.blocks[rel], half), self.cs.at[rel * 2 + half])


def weight_gathers(place, bufs, wo_own, wd_own, sems):
    wq, wu, wo, wd = bufs
    cols = wq.shape[1] // 2
    o_rows, d_rows, d_cols = wo.shape[2] // 2, wd.shape[3] // 2, wd.shape[4]
    specs = (
        (lambda row, half, core: wq.at[row, pl.ds(half * cols, cols), core], None),
        (lambda row, half, core: wu.at[row, pl.ds(half * cols, cols), core], None),
        (lambda row, half, core: wo.at[row, core, pl.ds(half * o_rows, o_rows)], lambda half: wo_own.at[pl.ds(half * o_rows, o_rows)]),
        *((lambda row, half, core, h=h: wd.at[h, row, core, pl.ds(half * d_rows, d_rows)],
           lambda half, h=h: wd_own.at[pl.ds(half * d_rows, d_rows), pl.ds(h * d_cols, d_cols)]) for h in range(2)),
    )
    return [Gather(place, blk, own, *(s.at[t] for s in sems)) for t, (blk, own) in enumerate(specs)]


def both_layers(side, x_ref, lens_ref, ln_ref, bq_ref, bo_ref, bu_ref, bd_ref, rot_ref, wq_ref, wu_ref, wo_ref, wd_ref,
                out_ref, wq1, wu1, wo1, wd1,
                wq, wu, wo, wd, xg, xg1, a_buf, m_buf, act, ctx, part, hop_a, hop_b, fin, q_stage, u_stage, q_own, u_own, vec_own, bias_own, bq_pad, vec_in, bias_in, vec, bq, bu,
                v_ss, v_rs, b_ss, b_rs, x_ss, x_rs, a_ss, a_rs, e_ss, e_rs, w_ss, w_rs, c_ss, c_rs, r_ss, r_rs, loc, loc1):
    f32, bf = jnp.float32, jnp.bfloat16
    place = Place(side)
    count = side * side * CORES
    seq, d_model = x_ref.shape
    head = rot_ref.shape[2]
    triple = 3 * head
    per = side
    ff = act.shape[2]
    half = seq // 2
    wide = wu_ref.shape[2] // (side * side)
    right, left = place.in_row(1), place.in_row(-1)
    nxt, prv, far = place.step(place.col, 1), place.step(place.col, -1), place.step(place.col, 2)

    second = place.core == 1
    width = head // CORES
    vec_own[...] = jnp.zeros_like(vec_own)
    for layer in range(2):
        vec_own[layer * 4:layer * 4 + 4, :width] = ln_ref[layer]
    vec_own[8:10, :width] = bo_ref[...].astype(f32)
    vec_own[10:12, :width] = bd_ref[...].astype(f32)
    vec_own[12:13, :width] = jnp.full((1, width), lens_ref[0].astype(f32))
    rows = vec_own[...]
    vec_own[...] = jnp.where(second, pltpu.roll(rows, width, 1), rows)
    bq_pad[...] = jnp.zeros_like(bq_pad)
    bq_pad[:, :3 * width] = bq_ref[...].astype(f32)
    lead, rest = bq_pad[:, :head], bq_pad[:, head:]
    lead_turned, rest_turned = pltpu.roll(lead, width, 1), pltpu.roll(rest, width, 1)
    upper = lax.broadcasted_iota(jnp.int32, lead.shape, 1) >= width
    q_tiles = (jnp.where(second, 0.0, lead), jnp.where(second, jnp.where(upper, lead_turned, 0.0), rest),
               jnp.where(second, jnp.where(upper, rest_turned, lead_turned), 0.0))
    tiles = wide // head
    bias_own[...] = jnp.zeros_like(bias_own)
    for layer in range(2):
        for t in range(3):
            bias_own[layer * 3 + t:layer * 3 + t + 1, :] = q_tiles[t][layer:layer + 1]
        for t in range(tiles):
            t_core, t_at = t // (tiles // CORES), t % (tiles // CORES)
            part_of = bu_ref[layer:layer + 1, t_at * head:(t_at + 1) * head].astype(f32)
            bias_own[6 + layer * tiles + t:7 + layer * tiles + t, :] = jnp.where(place.core == t_core, part_of, 0.0)

    barrier = pltpu.get_barrier_semaphore()
    others = [lax.rem(place.me + d, count) for d in range(1, count)]
    for dev in others:
        pl.semaphore_signal(barrier, inc=1, device_id={"fsdp": dev}, device_id_type=MESH)
    pl.semaphore_wait(barrier, count - 1)

    stages, own_stages = (q_stage, u_stage), (q_own, u_own)

    def exchange(layer, kind, dst_buf):
        src_ref, size = (wu_ref, wide) if kind else (wq_ref, triple)
        for d in (1, 3, 2, 0):
            col = place.step(place.col, d)
            dst = dst_buf.at[place.row, place.col, place.core]
            for k in range(side):
                off = pl.multiple_of((k * side + col) * size, size)
                src, to = src_ref.at[layer, :, pl.ds(off, size)], dst.at[:, pl.ds(k * size, size)]
                if d == 2:
                    way, at = k // 2, pl.ds(k % 2 * size, size)
                    send(src, stages[kind].at[layer, way, :, at], e_ss.at[layer, kind, way], e_rs.at[layer, kind, way], (right, left)[way])
                elif d:
                    send(src, to, a_ss.at[layer, kind, d], a_rs.at[layer, kind, d], place.in_row(d))
                elif layer:
                    pltpu.make_async_copy(src, own_stages[kind].at[:, pl.ds(k * size, size)], loc.at[4 + kind]).start()
                else:
                    pltpu.make_async_copy(src, to, a_rs.at[layer, kind, d]).start()

    def relay(layer, kind, dst_buf):
        for way, (origin, dev) in enumerate(((prv, right), (nxt, left))):
            piece = stages[kind].at[layer, way]
            settle(piece, e_rs.at[layer, kind, way])
            to = dst_buf.at[place.row, origin, place.core, :, pl.ds(way * piece.shape[1], piece.shape[1])]
            send(piece, to, a_ss.at[layer, kind, 2], a_rs.at[layer, kind, 2], dev)
        if layer:
            settle(own_stages[kind], loc.at[4 + kind])
            pltpu.make_async_copy(own_stages[kind], dst_buf.at[place.row, place.col, place.core], a_rs.at[layer, kind, 0]).start()

    def exchanged(layer, kind, dst_buf):
        for d in range(side):
            settle(dst_buf.at[place.row, place.step(place.col, -d), place.core], a_rs.at[layer, kind, d])

    gathers = [
        weight_gathers(place, (wq, wu, wo, wd), wo_ref.at[0], wd_ref.at[0], [s.at[0] for s in (w_ss, w_rs, c_ss, c_rs)]),
        weight_gathers(place, (wq1, wu1, wo1, wd1), wo_ref.at[1], wd_ref.at[1], [s.at[1] for s in (w_ss, w_rs, c_ss, c_rs)]),
    ]
    gq, gu, go, *gd = gathers[0]
    gq1, gu1, go1, *gd1 = gathers[1]
    d_cols = wd.shape[4]
    rows_of = lambda ref, col, h: ref.at[col, pl.ds(h * half, half)]
    x_ring = Ring(place, place.col, right, left, lambda col, h: rows_of(xg, col, h), lambda h: x_ref.at[pl.ds(h * half, half)], x_ss.at[0, 0], x_rs.at[0, 0])
    x1_at = lambda h: lambda col, half_at: xg1.at[col, pl.ds(half_at * half, half), pl.ds(h * d_cols, d_cols)]
    x1_rings = [Ring(place, place.col, right, left, x1_at(h), lambda half_at, h=h: x1_at(h)(place.col, half_at), x_ss.at[1, h], x_rs.at[1, h]) for h in range(2)]

    exchange(0, 0, wq)
    vec_at = lambda core, chip: vec_in.at[core, :, pl.ds(pl.multiple_of(chip * head, head), head)]
    bias_at = lambda core, row: bias_in.at[core, :, pl.ds(pl.multiple_of(row * head, head), head)]
    for d, dev in enumerate(others):
        send(vec_own, vec_at(place.core, place.chip), v_ss.at[d], v_rs.at[d], dev)
    column = [(e, c) for e in range(side) for c in range(CORES) if e or c]
    for i, (e, c) in enumerate(column):
        dev = place.dev(place.step(place.row, e), place.col, lax.rem(place.core + c, CORES))
        send(bias_own, bias_at(place.core, place.row), b_ss.at[i], b_rs.at[i], dev)
    for g in (go, gd[0]):
        g.start()
        g.own()
    relay(0, 0, wq)
    exchange(0, 1, wu)
    own = [(x_ref, xg.at[place.col]), (wo_ref.at[0], wo.at[place.row, place.core])]
    own += [(wd_ref.at[0, :, pl.ds(h * d_cols, d_cols)], wd.at[h, place.row, place.core]) for h in range(2)]
    for i, (src, dst) in enumerate(own):
        pltpu.make_async_copy(src, dst, loc.at[i]).start()

    vec_in[place.core, :, pl.ds(pl.multiple_of(place.chip * head, head), head)] = vec_own[...]
    bias_in[place.core, :, pl.ds(pl.multiple_of(place.row * head, head), head)] = bias_own[...]

    exchanged(0, 0, wq)
    gq.start()
    gq.own()
    relay(0, 1, wu)
    x_ring.start()
    exchanged(0, 1, wu)
    gq.forward()
    gu.start()
    gu.own()

    for d in range(1, count):
        src = lax.rem(place.me + count - d, count)
        settle(vec_at(lax.rem(src, CORES), src // CORES), v_rs.at[d - 1])
    for i, (e, c) in enumerate(column):
        settle(bias_at(lax.rem(place.core + c, CORES), place.step(place.row, -e)), b_rs.at[i])
    vec[...] = vec_in[0] + vec_in[1]
    for layer in range(2):
        for row in range(side):
            at = pl.ds(row * head, head)
            rows = bias_in[0, :, at] + bias_in[1, :, at]
            for tall, out, first, n in ((triple, bq, 0, 3), (wide, bu, 6, tiles)):
                for t in range(n):
                    i = first + layer * n + t
                    out[layer:layer + 1, row * tall + t * head:row * tall + (t + 1) * head] = rows[i:i + 1]

    x_ring.forward()
    exchange(1, 0, wq1)
    exchange(1, 1, wu1)
    go.forward()
    gq.hand()

    tile = min(32, half)

    def norm(src, doc, layer, to, halves=(0, 1)):
        par = [vec[layer * 4 + i:layer * 4 + i + 1, :] for i in range(4)]

        @pl.loop(halves[0] * half, (halves[-1] + 1) * half, step=tile)
        def _(r):
            at = pl.ds(r, tile)
            rows = src[doc, at, :].astype(f32)
            centered = rows - jnp.mean(rows, axis=-1, keepdims=True)
            var = jnp.mean(centered * centered, axis=-1, keepdims=True)
            normed = centered * lax.rsqrt(var + LN_EPS)
            to[at, :] = (normed * par[0] + par[1]).astype(bf)
            m_buf[doc, at, :] = (normed * par[2] + par[3]).astype(bf)

    def attend(doc, layer, rows):
        chip = place.row * side + doc
        lens = vec[12:13, pl.ds(pl.multiple_of(chip * head, head), head)]
        lane = lax.broadcasted_iota(jnp.int32, (1, head), 1)
        length = jnp.sum(jnp.where(lane == place.core * (head // CORES), lens, 0.0), axis=1, keepdims=True)
        query = lax.broadcasted_iota(jnp.int32, (seq, seq), 0)
        key = lax.broadcasted_iota(jnp.int32, (seq, seq), 1)
        visible = (key <= query) & (key.astype(f32) < length)
        pair = 2 * triple

        def turn(u):
            u = u.astype(f32)
            shift = head // 8
            return (u * rot_ref[0] + pltpu.roll(u, head - shift, 1) * rot_ref[1] + pltpu.roll(u, shift, 1) * rot_ref[2]).astype(bf)

        @pl.loop(0, per // 2)
        def _(p):
            at = pl.ds(pl.multiple_of(p * pair, pair), pair)
            w = wq[:, :, :, :, at].reshape(d_model, pair)
            qkv = (jnp.dot(rows[...], w, preferred_element_type=f32) + bq[layer:layer + 1, at]).astype(bf)
            for h in range(2):
                q, k, v = (qkv[:, h * triple + j * head:h * triple + (j + 1) * head] for j in range(3))
                scores = lax.dot_general(turn(q), turn(k), (((1,), (1,)), ((), ())), preferred_element_type=f32) * (head ** -0.5)
                scores = jnp.where(visible, scores, -1e30)
                probs = jnp.exp(scores - jnp.max(scores, axis=-1, keepdims=True))
                probs = (probs / jnp.sum(probs, axis=-1, keepdims=True)).astype(bf)
                to = pl.ds(pl.multiple_of((p * 2 + h) * head, head), head)
                ctx[doc, :, to] = jnp.dot(probs, v, preferred_element_type=f32).astype(bf)

    def up(doc, layer):
        step = ff // 8

        @pl.loop(0, 2)
        def _(n):
            for j in range(4):
                at = pl.ds(pl.multiple_of((n * 4 + j) * step, step), step)
                u = jnp.dot(m_buf[doc], wu[:, :, :, :, at].reshape(d_model, step), preferred_element_type=f32) + bu[layer:layer + 1, at]
                act[doc, :, at] = (0.5 * u * (1.0 + lax.erf(u * (0.5 ** 0.5)))).astype(bf)

    def down(doc, h):
        step = d_cols // 4
        for n in range(4):
            at = pl.ds(n * step, step)
            wide_at = pl.ds(pl.multiple_of(h * d_cols + n * step, step), step)
            tot = jnp.dot(ctx[doc], wo[:, :, :, wide_at].reshape(per * head, step), preferred_element_type=f32)
            part[doc, h, :, at] = tot + jnp.dot(act[doc], wd[h, :, :, :, at].reshape(ff, step), preferred_element_type=f32)

    top, low = pl.ds(0, half), pl.ds(half, half)

    def send_part(layer, h, i, doc, rows, to, dev):
        send(part.at[doc, h, rows], to.at[h], r_ss.at[layer, h, i], r_rs.at[layer, h, i], dev)

    def send_far(layer, h):
        send_part(layer, h, 0, far, top, hop_a, left)
        send_part(layer, h, 1, far, low, hop_b, right)

    def send_prv(layer, h):
        send_part(layer, h, 2, prv, low, fin.at[0], left)

    def send_nxt(layer, h):
        send_part(layer, h, 3, nxt, top, fin.at[1], right)

    def pass_on(layer, h):
        for i, hop, doc, first, dev in ((0, hop_a, prv, 0, left), (1, hop_b, nxt, half, right)):
            settle(hop.at[h], r_rs.at[layer, h, i])

            @pl.loop(0, half, step=tile)
            def _(r, hop=hop, doc=doc, first=first):
                hop[h, pl.ds(r, tile), :] = hop[h, pl.ds(r, tile), :] + part[doc, h, pl.ds(first + r, tile), :]

            send(hop.at[h], fin.at[2 + i, h], r_ss.at[layer, h, 4 + i], r_rs.at[layer, h, 4 + i], dev)

    def owner_sums(layer, src, store, done):
        for h in range(2):
            cols = slice(h * d_cols, (h + 1) * d_cols)
            for i in range(2, 6):
                settle(fin.at[i - 2, h], r_rs.at[layer, h, i])
            for first, f_one, f_two in ((0, 1, 2), (half, 0, 3)):
                @pl.loop(0, half, step=tile)
                def _(r, first=first, f_one=f_one, f_two=f_two):
                    here, at = pl.ds(r, tile), pl.ds(first + r, tile)
                    tot = part[place.col, h, at, :] + fin[f_one, h, here, :] + fin[f_two, h, here, :]
                    bias = vec[8 + layer:9 + layer, cols] + vec[10 + layer:11 + layer, cols]
                    store(at, cols, (src[place.col, at, cols].astype(f32) + (tot + bias)).astype(bf))

            done(h)

    def sums_sent(layer):
        for h in range(2):
            for i in range(6):
                settle(hop_a.at[h], r_ss.at[layer, h, i])

    def chosen(i, docs):
        doc = docs[-1]
        for at, other in enumerate(docs[:-1]):
            doc = jnp.where(i == at, other, doc)
        return doc

    mine = place.col
    nearest_first = (mine, nxt, prv, far)
    farthest_first = (far, nxt, prv, mine)

    settle(xg.at[place.col], loc.at[0])
    gq.tail()
    gq.take()

    @pl.loop(0, side)
    def _(i):
        doc = chosen(i, nearest_first)

        @pl.when(i == 1)
        def _():
            x_ring.rest()

        @pl.when(i == 2)
        def _():
            gu.forward()
            gd[0].forward()
            gd[1].start()
            gd[1].own()
            go.hand()

        @pl.when(i == 3)
        def _():
            x_ring.last()
            relay(1, 0, wq1)
            relay(1, 1, wu1)
            gu.hand()
            gd[0].hand()

        norm(xg, doc, 0, a_buf)
        attend(doc, 0, a_buf)

    go.tail()
    gu.tail()
    gu.take()
    settle(wo.at[place.row, place.core], loc.at[1])
    for h in range(2):
        settle(wd.at[h, place.row, place.core], loc.at[2 + h])

    def leave(i, h):
        for at, out in enumerate((send_far, send_nxt, send_prv)):
            @pl.when(i == at)
            def _(out=out):
                out(0, h)

    @pl.loop(0, side)
    def _(i):
        doc = chosen(i, farthest_first)
        up(doc, 0)

        @pl.when(i == 0)
        def _():
            gd[0].tail()
            go.take()
            gd[0].take()

        down(doc, 0)
        leave(i, 0)

        @pl.when(i == 1)
        def _():
            gd[1].forward()
            exchanged(1, 0, wq1)
            gq1.start()

        @pl.when(i == 2)
        def _():
            exchanged(1, 1, wu1)
            gu1.start()
            gd[1].hand()

    gd[1].tail()
    gd[1].take()

    @pl.loop(0, side)
    def _(i):
        down(chosen(i, farthest_first), 1)
        leave(i, 1)

    gq1.own()
    gu1.own()
    gq1.forward()
    pass_on(0, 0)
    gu1.forward()
    for g in (go1, gd1[0]):
        g.start()
        g.own()
    pass_on(0, 1)
    for g in gathers[0]:
        g.drain()
    gq1.hand()
    gq1.tail()
    gu1.hand()
    gq1.take()
    pltpu.make_async_copy(wq1, wq, loc1.at[0]).start()
    gu1.tail()
    gu1.take()
    pltpu.make_async_copy(wu1, wu, loc1.at[1]).start()

    def keep(at, cols, rows):
        xg1[place.col, at, cols] = rows

    owner_sums(0, xg, keep, lambda h: x1_rings[h].start())
    sums_sent(0)
    x_ring.drain()
    settle(wq, loc1.at[0])
    settle(wu, loc1.at[1])

    def load_rows(src, dst, own_src, sem):
        for e in range(side):
            for c in range(CORES):
                at = (place.step(place.row, e), lax.rem(place.core + c, CORES))
                pltpu.make_async_copy(src.at[at] if e or c else own_src, dst.at[at], sem).start()

    def load_down(h):
        load_rows(wd1.at[h], wd.at[h], wd_ref.at[1, :, pl.ds(h * d_cols, d_cols)], loc1.at[3 + h])

    norm(xg1, place.col, 1, xg.at[place.col])

    @pl.loop(0, side)
    def _(i):
        doc = chosen(i, nearest_first)

        @pl.when(i == 1)
        def _():
            for ring in x1_rings:
                ring.rest()
            norm(xg1, nxt, 1, xg.at[nxt], (0,))

        @pl.when(i == 3)
        def _():
            for ring in x1_rings:
                ring.last()
            norm(xg1, far, 1, xg.at[far])

        attend(doc, 1, xg.at[doc])

        @pl.when(i == 1)
        def _():
            for g in (go1, gd1[0]):
                g.hand()
                g.tail()

        @pl.when(i == 2)
        def _():
            gd1[1].hand()
            gd1[1].tail()

        up(doc, 1)

        @pl.when(i == 0)
        def _():
            go1.forward()
            gd1[0].forward()
            gd1[1].start()
            gd1[1].own()
            for ring in x1_rings:
                ring.forward()
            norm(xg1, nxt, 1, xg.at[nxt], (1,))
            norm(xg1, prv, 1, xg.at[prv], (0,))

        @pl.when(i == 1)
        def _():
            go1.take()
            load_rows(wo1, wo, wo_ref.at[1], loc1.at[2])
            gd1[0].take()
            load_down(0)
            norm(xg1, prv, 1, xg.at[prv], (1,))
            settle(wo, loc1.at[2])
            settle(wd.at[0], loc1.at[3])
            down(nxt, 0)
            send_nxt(1, 0)
            gd1[1].forward()

        @pl.when(i == 2)
        def _():
            gd1[1].take()
            load_down(1)
            down(prv, 0)
            send_prv(1, 0)
            settle(wd.at[1], loc1.at[4])
            down(nxt, 1)
            send_nxt(1, 1)
            down(prv, 1)
            send_prv(1, 1)

        @pl.when(i == 3)
        def _():
            for h in range(2):
                down(far, h)
                send_far(1, h)
            for h in range(2):
                down(place.col, h)

    pass_on(1, 0)
    pass_on(1, 1)

    def give_out(at, cols, rows):
        out_ref[at, cols] = rows

    owner_sums(1, xg1, give_out, lambda h: None)
    sums_sent(1)
    for g in gathers[1]:
        g.drain()
    for ring in x1_rings:
        ring.drain()
    for d in range(count - 1):
        settle(vec_own, v_ss.at[d])
    for i in range(len(column)):
        settle(bias_own, b_ss.at[i])
    for layer in range(2):
        for kind, buf in enumerate((wq, wu)):
            for d in range(1, side):
                settle(buf.at[0, 0, 0], a_ss.at[layer, kind, d])
            for way in range(2):
                settle(stages[kind].at[layer, way], e_ss.at[layer, kind, way])


VM = pl.BlockSpec(memory_space=pltpu.VMEM)
ANY = pl.BlockSpec(memory_space=pl.ANY)
DMA = pltpu.SemaphoreType.DMA


def solution(mesh):
    row_spec = P(('dp', 'fsdp'))
    inner = P(None, 'fsdp')
    in_specs = (row_spec, P(('dp', 'fsdp')), P(None, *inner)) + (inner,) * len(('w_qkv', 'b_qkv', 'w_out', 'b_out', 'w_up', 'b_up', 'w_down', 'b_down'))
    count = mesh.shape['fsdp']
    side = math.isqrt(count // CORES)

    def local_step(hidden_loc, lens_loc, ln_par, w_qkv, b_qkv, w_out, b_out, w_up, b_up, w_down, b_down):
        layers = ln_par.shape[0]
        _, seq_len, d_model = hidden_loc.shape
        d_rows, heads, triple = w_qkv.shape[1:]
        head_dim = triple // 3
        per = heads // side
        ff_rows = w_down.shape[1]
        ff = ff_rows * CORES * side
        bf, f32 = jnp.bfloat16, jnp.float32
        wq = w_qkv.reshape(layers, d_rows, heads * triple)
        bias_rows = -(-layers * (3 + ff // side // head_dim) // 16) * 16

        half = seq_len // 2
        wq_s, wu_s = (side, side, CORES, d_rows, per * triple), (side, side, CORES, d_rows, ff)
        wo_s, wd_s = (side, CORES) + w_out.shape[1:], (2, side, CORES, ff_rows, d_model // 2)
        outs = pl.pallas_call(
            functools.partial(both_layers, side),
            out_shape=(jax.ShapeDtypeStruct((seq_len, d_model), bf), *(jax.ShapeDtypeStruct(s, bf) for s in (wq_s, wu_s, wo_s, wd_s))),
            in_specs=[ANY, pl.BlockSpec(memory_space=pltpu.SMEM), VM, VM, VM, VM, VM, VM, ANY, ANY, ANY, ANY],
            out_specs=(VM, ANY, ANY, ANY, ANY),
            scratch_shapes=[
                *(pltpu.VMEM(s, bf) for s in (wq_s, wu_s, wo_s, wd_s)),
                pltpu.VMEM((side, seq_len, d_model), bf),
                pltpu.VMEM((side, seq_len, d_model), bf),
                pltpu.VMEM((seq_len, d_model), bf),
                pltpu.VMEM((side, seq_len, d_model), bf),
                pltpu.VMEM((side, seq_len, ff), bf),
                pltpu.VMEM((side, seq_len, per * head_dim), bf),
                pltpu.VMEM((side, 2, seq_len, d_model // 2), f32),
                pltpu.VMEM((2, half, d_model // 2), f32),
                pltpu.VMEM((2, half, d_model // 2), f32),
                pltpu.VMEM((4, 2, half, d_model // 2), f32),
                *(pltpu.VMEM((layers, 2, d_rows, cols // 2), bf) for cols in (per * triple, ff)),
                *(pltpu.VMEM((d_rows, cols), bf) for cols in (per * triple, ff)),
                pltpu.VMEM((16, head_dim), f32),
                pltpu.VMEM((bias_rows, head_dim), f32),
                pltpu.VMEM((layers, 2 * head_dim), f32),
                pltpu.VMEM((CORES, 16, d_model), f32),
                pltpu.VMEM((CORES, bias_rows, side * head_dim), f32),
                pltpu.VMEM((16, d_model), f32),
                pltpu.VMEM((layers, per * triple), f32),
                pltpu.VMEM((layers, ff), f32),
                *([DMA((count - 1,))] * 2), *([DMA((side * CORES - 1,))] * 2),
                *([DMA((layers, 2, 6))] * 2), *([DMA((layers, 2, side))] * 2), *([DMA((layers, 2, 2))] * 2),
                *([DMA((layers, 5, 6))] * 2), *([DMA((layers, 5, 8))] * 2),
                *([DMA((layers, 2, 6))] * 2), DMA((7,)), DMA((5,)),
            ],
            compiler_params=pltpu.CompilerParams(collective_id=0, has_side_effects=True, vmem_limit_bytes=67043328),
        )(hidden_loc[0], lens_loc, ln_par, b_qkv, b_out, b_up, b_down, rotary_factors(seq_len, head_dim), wq, w_up, w_out, w_down)
        return outs[0][None]

    return jax.shard_map(local_step, mesh=mesh, in_specs=in_specs, out_specs=row_spec, check_vma=False)
```
